128 devices in a mesh: section: 4 (over x), fsdp: 32 (over y, z, core).
Axes of the slice: x: 4, y: 4, z: 4, core: 2. Of those that a mesh axis runs over, the one named last changes fastest.
Arguments:
- grad_parts: bfloat16 [4, 32, 8192, 1024], P('section', 'fsdp'), may hold values from -510 to 510
- first_codes: int32 [4, 8192, 1024], P('section', 'fsdp'), may hold values from -7 to 7
- first_rows: float32 [4, 8192], P('section', 'fsdp'), may hold values from 0.003 to 0.03
- first_columns: float32 [4, 1024], P('section'), may hold values from 0.003 to 0.03
- second_codes: int32 [4, 8192, 1024], P('section', 'fsdp'), may hold values from 1 to 15
- second_rows: float32 [4, 8192], P('section', 'fsdp'), may hold values from 0.001 to 0.01
- second_columns: float32 [4, 1024], P('section'), may hold values from 0.001 to 0.01
Outputs:
- direction: float32 [4, 8192, 1024], P('section', 'fsdp')
- first_scaled: float32 [4, 8192, 1024], P('section', 'fsdp')
- second_scaled: float32 [4, 8192, 1024], P('section', 'fsdp')
- first_rowmax: float32 [4, 8192], P('section', 'fsdp')
- first_colmax: float32 [4, 1024], P('section')
- second_rowmax: float32 [4, 8192], P('section', 'fsdp')
- second_colmax: float32 [4, 1024], P('section')
The draws below stay inside these ranges and needn't reach their ends.
All inputs are finite; a program needn't handle non-finite values. Where the reference program divides by a largest or mean magnitude, that divisor is 1e-20 or more.
Results may differ from the reference program's by a relative error of at most 0.0003.
Values may be sent and summed in bfloat16 or wider, within the bound.
A program may use at most 192 MiB of HBM per device.

```python
import math
import jax
import jax.numpy as jnp
from jax import lax

ROWS = 8192
KV = 1024
LAYERS_ALL = 4
PARTIALS = 32


def draw_grad_parts(key, part):
    subkeys = jax.random.split(key, 5)
    full_shape = (LAYERS_ALL, PARTIALS, ROWS, KV)
    col_scale = jnp.exp(jax.random.uniform(subkeys[0], (LAYERS_ALL, 1, 1, KV), jnp.float32, math.log(0.2), math.log(5.0)))
    row_scale = jnp.exp(jax.random.uniform(subkeys[1], (LAYERS_ALL, 1, ROWS, 1), jnp.float32, math.log(0.5), math.log(2.0)))
    owner_block = jax.random.randint(subkeys[2], (LAYERS_ALL, PARTIALS, 1, 1), 0, PARTIALS)
    row_block = (jnp.arange(ROWS, dtype=jnp.int32) // (ROWS // PARTIALS)).reshape(1, 1, ROWS, 1)
    spike_gain = jnp.where(row_block == owner_block, 4.0, 1.0)
    basis_values = jnp.clip(jax.random.normal(subkeys[3], full_shape, jnp.float32), -6.0, 6.0)
    return (basis_values * col_scale * row_scale * spike_gain).astype(jnp.bfloat16)


def plant(result, key, least, high):
    longest = result.shape.index(max(result.shape))
    spots = []
    for shift in (0, 1):
        where = [jax.random.randint(jax.random.fold_in(key, axis), (), 0, length) for axis, length in enumerate(result.shape)]
        where[longest] = (where[longest] + shift) % result.shape[longest]
        spots.append(tuple(where))
    return result.at[spots[0]].set(least).at[spots[1]].set(high)


def shard_levels(rng, extent, cuts, least, largest):
    factor_of = 1.0
    for position, shards_of in cuts:
        heights = jax.random.uniform(jax.random.fold_in(jax.random.fold_in(rng, 6), position), (shards_of,), jnp.float32, least / len(cuts), largest / len(cuts))
        factor_of = factor_of * jnp.repeat(jnp.exp(heights), extent[position] // shards_of).reshape((-1,) + (1,) * (len(extent) - 1 - position))
    return factor_of


def setup_inputs(seed: int = 0) -> dict:
    keys = jax.random.split(jax.random.key(seed), 8)
    return {
        "grad_parts": draw_grad_parts(jax.random.fold_in(keys[7], 71), 0),
        "first_codes": plant(jax.random.randint(keys[1], (LAYERS_ALL, ROWS, KV), -7, 8), jax.random.fold_in(keys[1], 1), -7, 7).astype(jnp.int32),
        "first_rows": jnp.clip(jnp.exp(math.log(0.03) - 2.3025851 * jax.random.uniform(keys[2], (LAYERS_ALL, ROWS), jnp.float32) ** shard_levels(keys[2], (LAYERS_ALL, ROWS), ((0, 4), (1, 32)), -0.2, 0.2)), 0.003, 0.03),
        "first_columns": jnp.clip(jnp.exp(math.log(0.03) - 2.3025851 * jax.random.uniform(keys[3], (LAYERS_ALL, KV), jnp.float32) ** shard_levels(keys[3], (LAYERS_ALL, KV), ((0, 4),), -0.2, 0.2)), 0.003, 0.03),
        "second_codes": plant(jax.random.randint(keys[4], (LAYERS_ALL, ROWS, KV), 1, 16), jax.random.fold_in(keys[4], 1), 1, 15).astype(jnp.int32),
        "second_rows": jnp.clip(jnp.exp(math.log(0.01) - 2.30258502 * jax.random.uniform(keys[5], (LAYERS_ALL, ROWS), jnp.float32) ** shard_levels(keys[5], (LAYERS_ALL, ROWS), ((0, 4), (1, 32)), -0.2, 0.2)), 0.001, 0.01),
        "second_columns": jnp.clip(jnp.exp(math.log(0.01) - 2.30258502 * jax.random.uniform(keys[6], (LAYERS_ALL, KV), jnp.float32) ** shard_levels(keys[6], (LAYERS_ALL, KV), ((0, 4),), -0.2, 0.2)), 0.001, 0.01),
    }


beta_first = 0.9
beta_second = 0.999
clip_rms = 3.0
epsilon = 1e-08
scale_floor = 0.001

def dequantize(code_values, levels, row_scale, col_scale):
    scale_bound = jnp.minimum(row_scale[:, :, None], col_scale[:, None, :])
    return code_values.astype(jnp.float32) / levels * scale_bound

def moments(gradient, clip_scale, first_codes, first_rows, first_columns, second_codes, second_rows, second_columns):
    first_old = dequantize(first_codes, 7.0, first_rows, first_columns)
    second_old = dequantize(second_codes, 15.0, second_rows, second_columns)
    clipped = clip_scale * gradient
    first_new = beta_first * first_old + (1.0 - beta_first) * clipped
    second_new = beta_second * second_old + (1.0 - beta_second) * clipped * clipped
    direction = first_new / (jnp.sqrt(second_new) + epsilon)
    return (first_new, second_new, direction)

def reference(grad_parts, first_codes, first_rows, first_columns, second_codes, second_rows, second_columns):

    def add_part(which_part, running):
        partial_value = lax.dynamic_index_in_dim(grad_parts, which_part, 1, keepdims=False)
        return running + partial_value.astype(jnp.float32)
    gradient = lax.fori_loop(0, PARTIALS, add_part, jnp.zeros((LAYERS_ALL, ROWS, KV), jnp.float32))
    square_sum = jnp.sum(gradient * gradient)
    clip_limit = clip_rms * math.sqrt(LAYERS_ALL * ROWS * KV)
    clip_scale = clip_limit / jnp.maximum(jnp.sqrt(square_sum), clip_limit)
    first_new, second_new, direction = moments(gradient, clip_scale, first_codes, first_rows, first_columns, second_codes, second_rows, second_columns)
    first_rowmax = jnp.maximum(lax.optimization_barrier(jnp.max(jnp.abs(first_new), axis=2)), scale_floor)
    first_colmax = jnp.maximum(lax.optimization_barrier(jnp.max(jnp.abs(first_new), axis=1)), scale_floor)
    second_rowmax = lax.optimization_barrier(jnp.max(second_new, axis=2))
    second_colmax = lax.optimization_barrier(jnp.max(second_new, axis=1))
    first_scaled = first_new / jnp.minimum(first_rowmax[:, :, None], first_colmax[:, None, :])
    second_scaled = second_new / jnp.minimum(second_rowmax[:, :, None], second_colmax[:, None, :])
    return (direction, first_scaled, second_scaled, first_rowmax, first_colmax, second_rowmax, second_colmax)
```

```python
import functools
import math

import jax
import jax.numpy as jnp
from jax import lax
from jax.experimental import pallas as pl
from jax.experimental.pallas import tpu as pltpu
from jax.sharding import Mesh
from jax.sharding import PartitionSpec as P

Y, Z, C, X = "fsdp_0", "fsdp_1", "fsdp_2", "section"
FSDP = (Y, Z, C)
MESH = pl.DeviceIdType.MESH

beta_first = 0.9
beta_second = 0.999
clip_rms = 3.0
epsilon = 1e-08
scale_floor = 0.001

SLICES = 8
DIRS = ((0, 1), (1, 3))


def remote(src, dst, send, recv, device):
    return pltpu.make_async_remote_copy(
        src_ref=src, dst_ref=dst, send_sem=send, recv_sem=recv,
        device_id=device, device_id_type=MESH,
    )


def landed(buf, sem):
    pltpu.make_async_copy(buf, buf, sem).wait()


def kernel(
    clip_limit,
    grads, first_codes, first_rows, first_columns, second_codes, second_rows, second_columns,
    first_new, second_new, first_rowmax, first_colmax, second_rowmax, second_colmax,
    own, got, send_l, recv_l, send_m, recv_m, total, recv_l2, send_m2, recv_m2,
    codes, grad, squares, norm_x, norm_y, norm_z, rowmax, colmax, col_y, col_z,
    own_sem, got_sem, code_sem, l_sem, m_sem, l2_sem, m2_sem, small_sem,
    got_send, l_send, m_send, l2_send, m2_send, small_send,
):
    slices, _, _, rows, width = own.shape
    quarter = width // 4
    y, z, c, x = (lax.axis_index(a) for a in (Y, Z, C, X))
    at = (y, z)
    names = (Y, Z)
    other = 1 - c

    def step(v, k):
        return lax.rem(v + k, 4)

    for i, ref in enumerate((first_codes, second_codes)):
        pltpu.make_async_copy(ref, codes.at[i], code_sem.at[i]).start()

    def load(p, _):
        pltpu.make_async_copy(
            grads.at[:, :, c, pl.ds(p * rows, rows), :], own.at[p], own_sem.at[p]
        ).start()
        return _

    lax.fori_loop(0, slices, load, 0)

    barrier = pltpu.get_barrier_semaphore()
    peers = [{C: other}]
    for axis, name in enumerate(names):
        for k in (1, 3):
            peers.append({name: step(at[axis], k)})
    for k in (1, 2, 3):
        peers.append({X: step(x, k)})
    for peer in peers:
        pl.semaphore_signal(barrier, inc=1, device_id=peer, device_id_type=MESH)
    pl.semaphore_wait(barrier, len(peers))

    def give(p, _):
        remote(
            grads.at[:, :, other, pl.ds(p * rows, rows), :], got.at[p],
            got_send, got_sem.at[p], {C: other},
        ).start()
        return _

    lax.fori_loop(0, slices, give, 0)

    def columns(axis, slot):
        return pl.ds((2 * axis + slot) * quarter, quarter)

    def pair(p, axis, index, slot):
        where = (p, index, slice(None)) if axis == 0 else (p, slice(None), index)
        where = (*where, slice(None), columns(axis, slot))
        return own[where].astype(jnp.float32) + got[where].astype(jnp.float32)

    def leaves(p, _):
        landed(own.at[p], own_sem.at[p])
        landed(got.at[p], got_sem.at[p])
        for axis in (0, 1):
            me = at[axis]
            for slot, k in DIRS:
                send_l[p, axis, slot, 0] = pair(p, axis, step(me, 2), slot)
                send_l[p, axis, slot, 1] = pair(p, axis, step(me, k), 1 - slot)
                remote(
                    send_l.at[p, axis, slot], recv_l.at[p, axis, slot],
                    l_send, l_sem.at[p, axis, slot], {names[axis]: step(me, k)},
                ).start()
        return _

    lax.fori_loop(0, slices, leaves, 0)

    def middles(p, _):
        for axis in (0, 1):
            me = at[axis]
            for slot, k in DIRS:
                landed(recv_l.at[p, axis, slot], l_sem.at[p, axis, slot])
                send_m[p, axis, slot] = pair(p, axis, step(me, k), slot) + recv_l[p, axis, slot, 0]
                remote(
                    send_m.at[p, axis, slot], recv_m.at[p, axis, slot],
                    m_send, m_sem.at[p, axis, slot], {names[axis]: step(me, k)},
                ).start()
        return _

    lax.fori_loop(0, slices, middles, 0)

    for i, ref in enumerate((first_codes, second_codes)):
        pltpu.make_async_copy(ref, codes.at[i], code_sem.at[i]).wait()
    for i, (row_ref, col_ref, out, factor) in enumerate((
        (first_rows, first_columns, first_new, beta_first / 7.0),
        (second_rows, second_columns, second_new, beta_second / 15.0),
    )):
        row_count = row_ref.shape[1]
        by_row = jnp.transpose(jnp.broadcast_to(row_ref[...], (128, row_count)))
        for j in range(width // 128):
            cols = pl.ds(j * 128, 128)
            bound = jnp.minimum(by_row, col_ref[:, cols])
            out[:, cols] = codes[i, :, cols].astype(jnp.float32) * factor * bound

    def totals(p, _):
        for axis in (0, 1):
            me, over, across = at[axis], at[1 - axis], names[1 - axis]
            for slot, k in DIRS:
                landed(recv_m.at[p, axis, slot], m_sem.at[p, axis, slot])
                total[p, axis, slot] = (
                    pair(p, axis, me, slot) + recv_m[p, axis, slot] + recv_l[p, axis, 1 - slot, 1]
                )
            for slot, k in DIRS:
                for unit, (which, index) in enumerate(((slot, 2), (1 - slot, k))):
                    remote(
                        total.at[p, axis, which, step(over, index)], recv_l2.at[p, axis, slot, unit],
                        l2_send, l2_sem.at[p, axis, slot], {across: step(over, k)},
                    ).start()
        return _

    lax.fori_loop(0, slices, totals, 0)

    def middles2(p, _):
        for axis in (0, 1):
            over, across = at[1 - axis], names[1 - axis]
            for slot, k in DIRS:
                landed(recv_l2.at[p, axis, slot], l2_sem.at[p, axis, slot])
                send_m2[p, axis, slot] = (
                    total[p, axis, slot, step(over, k)] + recv_l2[p, axis, slot, 0]
                )
                remote(
                    send_m2.at[p, axis, slot], recv_m2.at[p, axis, slot],
                    m2_send, m2_sem.at[p, axis, slot], {across: step(over, k)},
                ).start()
        return _

    lax.fori_loop(0, slices, middles2, 0)

    squares[...] = jnp.zeros_like(squares)

    def finish(p, _):
        for axis in (0, 1):
            over = at[1 - axis]
            for slot, k in DIRS:
                landed(recv_m2.at[p, axis, slot], m2_sem.at[p, axis, slot])
                value = (
                    total[p, axis, slot, over] + recv_m2[p, axis, slot]
                    + recv_l2[p, axis, 1 - slot, 1]
                )
                grad[pl.ds(pl.multiple_of(p * rows, rows), rows), columns(axis, slot)] = value
                sq = value * value
                part = sq[:, :128]
                for j in range(1, quarter // 128):
                    part = part + sq[:, j * 128 : (j + 1) * 128]
                squares[...] += jnp.sum(part.reshape(rows // 8, 8, 128), axis=0)
        return _

    lax.fori_loop(0, slices, finish, 0)

    def exchange(value_ref, slots, targets, sem):
        for i, target in enumerate(targets):
            remote(value_ref, slots.at[i], small_send.at[sem], small_sem.at[sem], target).start()

    x_peers = [{X: step(x, k)} for k in (1, 2, 3)]
    y_peers = [
        {Y: step(y, ky), C: (other if kc else c)}
        for ky in range(4) for kc in range(2) if ky or kc
    ]
    z_peers = [{Z: step(z, k)} for k in (1, 2, 3)]

    for i, (slots, targets) in enumerate(((norm_x, x_peers), (norm_y, y_peers), (norm_z, z_peers))):
        exchange(squares, slots, targets, i)
        landed(slots, small_sem.at[i])
        pltpu.make_async_copy(slots, slots, small_send.at[i]).wait()
        squares[...] += jnp.sum(slots[...], axis=0)

    square_sum = jnp.sum(squares[...], keepdims=True)
    clip_scale = clip_limit / jnp.maximum(jnp.sqrt(square_sum), clip_limit)

    tile = 32
    first_top = jnp.zeros((8, width), jnp.float32)
    second_top = jnp.zeros((8, width), jnp.float32)

    def moment(t, tops):
        here = pl.ds(pl.multiple_of(t * tile, tile), tile)
        clipped = clip_scale * grad[here, :]
        first = first_new[here, :] + (1.0 - beta_first) * clipped
        second = second_new[here, :] + (1.0 - beta_second) * clipped * clipped
        first_new[here, :] = first
        second_new[here, :] = second
        outs = []
        for i, (value, top) in enumerate(((jnp.abs(first), tops[0]), (second, tops[1]))):
            outs.append(jnp.maximum(top, jnp.max(value.reshape(tile // 8, 8, width), axis=0)))
            most = value[:, :128]
            for j in range(1, width // 128):
                most = jnp.maximum(most, value[:, j * 128 : (j + 1) * 128])
            rowmax[i, here, :] = most
        return tuple(outs)

    first_top, second_top = lax.fori_loop(0, grad.shape[0] // tile, moment, (first_top, second_top))
    colmax[0:1, :] = jnp.max(first_top, axis=0, keepdims=True)
    colmax[1:2, :] = jnp.max(second_top, axis=0, keepdims=True)

    exchange(colmax, col_y, y_peers, 3)
    first_row = jnp.max(jnp.transpose(rowmax[0]), axis=0, keepdims=True)
    first_rowmax[...] = jnp.maximum(first_row, scale_floor)
    second_rowmax[...] = jnp.max(jnp.transpose(rowmax[1]), axis=0, keepdims=True)
    landed(col_y, small_sem.at[3])
    pltpu.make_async_copy(col_y, col_y, small_send.at[3]).wait()
    colmax[...] = jnp.maximum(colmax[...], jnp.max(col_y[...], axis=0))
    exchange(colmax, col_z, z_peers, 4)
    landed(col_z, small_sem.at[4])
    result = jnp.maximum(colmax[...], jnp.max(col_z[...], axis=0))
    first_colmax[...] = jnp.maximum(result[0:1], scale_floor)
    second_colmax[...] = result[1:2]
    pltpu.make_async_copy(col_z, col_z, small_send.at[4]).wait()

    landed(got, got_send)
    landed(send_l, l_send)
    landed(send_m, m_send)
    landed(recv_l2, l2_send)
    landed(send_m2, m2_send)


def local(
    grad_parts, first_codes, first_rows, first_columns, second_codes, second_rows, second_columns
):
    layer_count, _, row_count, col_count = grad_parts.shape
    entries = layer_count * lax.axis_size(X) * row_count * col_count
    clip_limit = clip_rms * math.sqrt(entries)
    own_rows = first_codes.shape[1]
    rows = own_rows // SLICES
    q = col_count // 4
    f32, bf16 = jnp.float32, jnp.bfloat16
    shape = jax.ShapeDtypeStruct
    vmem = pltpu.VMEM
    dma = pltpu.SemaphoreType.DMA
    grads = grad_parts.reshape(4, 4, 2, own_rows, col_count)
    any_spec = pl.BlockSpec(memory_space=pl.ANY)
    vmem_spec = pl.BlockSpec(memory_space=pltpu.VMEM)
    n = SLICES
    first_new, second_new, first_rowmax, first_colmax, second_rowmax, second_colmax = pl.pallas_call(
        functools.partial(kernel, clip_limit),
        out_shape=(
            shape((own_rows, col_count), f32), shape((own_rows, col_count), f32),
            shape((1, own_rows), f32), shape((1, col_count), f32),
            shape((1, own_rows), f32), shape((1, col_count), f32),
        ),
        in_specs=[any_spec, any_spec, vmem_spec, vmem_spec, any_spec, vmem_spec, vmem_spec],
        out_specs=[vmem_spec] * 6,
        scratch_shapes=[
            vmem((n, 4, 4, rows, col_count), bf16),
            vmem((n, 4, 4, rows, col_count), bf16),
            vmem((n, 2, 2, 2, 4, rows, q), f32),
            vmem((n, 2, 2, 2, 4, rows, q), f32),
            vmem((n, 2, 2, 4, rows, q), f32),
            vmem((n, 2, 2, 4, rows, q), f32),
            vmem((n, 2, 2, 4, rows, q), f32),
            vmem((n, 2, 2, 2, rows, q), f32),
            vmem((n, 2, 2, rows, q), f32),
            vmem((n, 2, 2, rows, q), f32),
            vmem((2, own_rows, col_count), jnp.int32),
            vmem((own_rows, col_count), f32),
            vmem((8, 128), f32),
            vmem((3, 8, 128), f32),
            vmem((7, 8, 128), f32),
            vmem((3, 8, 128), f32),
            vmem((2, own_rows, 128), f32),
            vmem((2, col_count), f32),
            vmem((7, 2, col_count), f32),
            vmem((3, 2, col_count), f32),
            dma((n,)), dma((n,)), dma((2,)),
            dma((n, 2, 2)), dma((n, 2, 2)), dma((n, 2, 2)), dma((n, 2, 2)), dma((5,)),
            dma, dma, dma, dma, dma, dma((5,)),
        ],
        compiler_params=pltpu.CompilerParams(
            collective_id=0, has_side_effects=True, vmem_limit_bytes=67043328
        ),
        name="clipped_adam",
    )(
        grads, first_codes[0], first_rows, first_columns, second_codes[0], second_rows,
        second_columns,
    )
    direction = first_new / (jnp.sqrt(second_new) + epsilon)
    first_scaled = first_new / jnp.minimum(first_rowmax[0, :, None], first_colmax)
    second_scaled = second_new / jnp.minimum(second_rowmax[0, :, None], second_colmax)
    return (
        direction[None], first_scaled[None], second_scaled[None],
        first_rowmax, first_colmax, second_rowmax, second_colmax,
    )


def solution(mesh):
    torus = Mesh(mesh.devices.reshape(mesh.shape["section"], 4, 4, 2), (X, Y, Z, C))
    placed = (
        P(X, FSDP, None, None),
        P(X, FSDP, None),
        P(X, FSDP),
        P(X, None),
        P(X, FSDP, None),
        P(X, FSDP),
        P(X, None),
    )
    return jax.shard_map(
        local,
        mesh=torus,
        in_specs=placed,
        out_specs=(
            P(X, FSDP, None), P(X, FSDP, None), P(X, FSDP, None),
            P(X, FSDP), P(X, None), P(X, FSDP), P(X, None),
        ),
        check_vma=False,
    )
```

```python
import functools
import math

import jax
import jax.numpy as jnp
from jax import lax
from jax.experimental import pallas as pl
from jax.experimental.pallas import tpu as pltpu
from jax.sharding import Mesh
from jax.sharding import PartitionSpec as P

Y, Z, C, X = "fsdp_0", "fsdp_1", "fsdp_2", "section"
FSDP = (Y, Z, C)
MESH = pl.DeviceIdType.MESH

beta_first = 0.9
beta_second = 0.999
clip_rms = 3.0
epsilon = 1e-08
scale_floor = 0.001

SLICES = 8
LEVELS = 32766.0
TINY = 2e-34
DIRS = ((0, 1), (1, 3))


def remote(src, dst, send, recv, device):
    return pltpu.make_async_remote_copy(
        src_ref=src, dst_ref=dst, send_sem=send, recv_sem=recv,
        device_id=device, device_id_type=MESH,
    )


def landed(buf, sem):
    pltpu.make_async_copy(buf, buf, sem).wait()


def put(value, codes, tops, key):
    top = jnp.maximum(jnp.max(jnp.abs(value), axis=0, keepdims=True), TINY)
    scaled = jnp.round(value * (LEVELS / top))
    codes[key] = scaled.astype(jnp.int32).astype(jnp.int16)
    *lead, row = key
    tops[(*lead, pl.ds(row, 1))] = top


def take(codes, tops, key):
    *lead, row = key
    unit = tops[(*lead, pl.ds(row, 1))] * (1.0 / LEVELS)
    return codes[key].astype(jnp.int32).astype(jnp.float32) * unit


def kernel(
    clip_limit,
    grads, first_codes, first_rows, first_columns, second_codes, second_rows, second_columns,
    first_new, second_new, first_rowmax, first_colmax, second_rowmax, second_colmax,
    own, got, sent_l, sent_lt, came_l, came_lt, sent_m, sent_mt, came_m, came_mt, total,
    sent_l2, sent_l2t, came_l2, came_l2t, sent_m2, sent_m2t, came_m2, came_m2t,
    codes, grad, squares, norm_x, norm_y, norm_z, rowmax, colmax, col_y, col_z,
    own_sem, got_sem, code_sem, l_sem, m_sem, l2_sem, m2_sem, small_sem,
    got_send, sends, small_send,
):
    slices, _, _, rows, width = own.shape
    quarter = width // 4
    y, z, c, x = (lax.axis_index(a) for a in (Y, Z, C, X))
    at = (y, z)
    names = (Y, Z)
    other = 1 - c

    def step(v, k):
        return lax.rem(v + k, 4)

    def load(p, _):
        pltpu.make_async_copy(
            grads.at[:, :, c, pl.ds(p * rows, rows), :], own.at[p], own_sem.at[p]
        ).start()
        return _

    lax.fori_loop(0, slices, load, 0)
    for i, ref in enumerate((first_codes, second_codes)):
        pltpu.make_async_copy(ref, codes.at[i], code_sem.at[i]).start()

    barrier = pltpu.get_barrier_semaphore()
    peers = [{C: other}]
    for axis, name in enumerate(names):
        for k in (1, 3):
            peers.append({name: step(at[axis], k)})
    for k in (1, 2, 3):
        peers.append({X: step(x, k)})
    for peer in peers:
        pl.semaphore_signal(barrier, inc=1, device_id=peer, device_id_type=MESH)
    pl.semaphore_wait(barrier, len(peers))

    def give(p, _):
        remote(
            grads.at[:, :, other, pl.ds(p * rows, rows), :], got.at[p],
            got_send, got_sem.at[p], {C: other},
        ).start()
        return _

    lax.fori_loop(0, slices, give, 0)

    def columns(axis, slot):
        return pl.ds((2 * axis + slot) * quarter, quarter)

    def pair(p, axis, index, j, slot):
        where = (p, index, j) if axis == 0 else (p, j, index)
        where = (*where, slice(None), columns(axis, slot))
        return own[where].astype(jnp.float32) + got[where].astype(jnp.float32)

    def send(kind, key, ref, ref_t, out, out_t, sem, device):
        remote(ref.at[key], out.at[key], sends.at[kind], sem.at[(*key, 0)], device).start()
        remote(ref_t.at[key], out_t.at[key], sends.at[kind + 4], sem.at[(*key, 1)], device).start()

    def arrived(key, ref, ref_t, sem):
        landed(ref.at[key], sem.at[(*key, 0)])
        landed(ref_t.at[key], sem.at[(*key, 1)])

    def leaves(p, _):
        landed(own.at[p], own_sem.at[p])
        landed(got.at[p], got_sem.at[p])
        for axis in (0, 1):
            me = at[axis]
            for slot, k in DIRS:
                for j in range(4):
                    value = pair(p, axis, step(me, 2), j, slot)
                    put(value, sent_l, sent_lt, (p, axis, slot, j))
                    value = pair(p, axis, step(me, k), j, 1 - slot)
                    put(value, sent_l, sent_lt, (p, axis, slot, 4 + j))
                send(0, (p, axis, slot), sent_l, sent_lt, came_l, came_lt, l_sem,
                     {names[axis]: step(me, k)})
        return _

    lax.fori_loop(0, slices, leaves, 0)

    for i, ref in enumerate((first_codes, second_codes)):
        pltpu.make_async_copy(ref, codes.at[i], code_sem.at[i]).wait()
    for i, (row_ref, col_ref, out, factor) in enumerate((
        (first_rows, first_columns, first_new, beta_first / 7.0),
        (second_rows, second_columns, second_new, beta_second / 15.0),
    )):
        row_count = row_ref.shape[1]
        by_row = jnp.transpose(jnp.broadcast_to(row_ref[...], (128, row_count)))
        for j in range(width // 128):
            cols = pl.ds(j * 128, 128)
            bound = jnp.minimum(by_row, col_ref[:, cols])
            out[:, cols] = codes[i, :, cols].astype(jnp.float32) * factor * bound

    def middles(p, _):
        for axis in (0, 1):
            me = at[axis]
            for slot, k in DIRS:
                key = (p, axis, slot)
                arrived(key, came_l, came_lt, l_sem)
                for j in range(4):
                    value = pair(p, axis, step(me, k), j, slot)
                    value = value + take(came_l, came_lt, (*key, j))
                    put(value, sent_m, sent_mt, (*key, j))
                send(1, key, sent_m, sent_mt, came_m, came_mt, m_sem, {names[axis]: step(me, k)})
        return _

    lax.fori_loop(0, slices, middles, 0)

    def totals(p, _):
        for axis in (0, 1):
            me, over, across = at[axis], at[1 - axis], names[1 - axis]
            for slot, k in DIRS:
                arrived((p, axis, slot), came_m, came_mt, m_sem)
                for j in range(4):
                    total[p, axis, slot, j] = (
                        pair(p, axis, me, j, slot)
                        + take(came_m, came_mt, (p, axis, slot, j))
                        + take(came_l, came_lt, (p, axis, 1 - slot, 4 + j))
                    )
            for slot, k in DIRS:
                for unit, (which, index) in enumerate(((slot, 2), (1 - slot, k))):
                    value = total[p, axis, which, step(over, index)]
                    put(value, sent_l2, sent_l2t, (p, axis, slot, unit))
                send(2, (p, axis, slot), sent_l2, sent_l2t, came_l2, came_l2t, l2_sem,
                     {across: step(over, k)})
        return _

    lax.fori_loop(0, slices, totals, 0)

    def middles2(p, _):
        for axis in (0, 1):
            over, across = at[1 - axis], names[1 - axis]
            for slot, k in DIRS:
                key = (p, axis, slot)
                arrived(key, came_l2, came_l2t, l2_sem)
                value = total[p, axis, slot, step(over, k)] + take(came_l2, came_l2t, (*key, 0))
                put(value, sent_m2, sent_m2t, (*key, 0))
                send(3, key, sent_m2, sent_m2t, came_m2, came_m2t, m2_sem, {across: step(over, k)})
        return _

    lax.fori_loop(0, slices, middles2, 0)

    squares[...] = jnp.zeros_like(squares)

    def finish(p, _):
        for axis in (0, 1):
            over = at[1 - axis]
            for slot, k in DIRS:
                arrived((p, axis, slot), came_m2, came_m2t, m2_sem)
                value = (
                    total[p, axis, slot, over]
                    + take(came_m2, came_m2t, (p, axis, slot, 0))
                    + take(came_l2, came_l2t, (p, axis, 1 - slot, 1))
                )
                grad[pl.ds(pl.multiple_of(p * rows, rows), rows), columns(axis, slot)] = value
                sq = value * value
                part = sq[:, :128]
                for j in range(1, quarter // 128):
                    part = part + sq[:, j * 128 : (j + 1) * 128]
                squares[...] += jnp.sum(part.reshape(rows // 8, 8, 128), axis=0)
        return _

    lax.fori_loop(0, slices, finish, 0)

    def exchange(value_ref, slots, targets, sem):
        for i, target in enumerate(targets):
            remote(value_ref, slots.at[i], small_send.at[sem], small_sem.at[sem], target).start()

    x_peers = [{X: step(x, k)} for k in (1, 2, 3)]
    y_peers = [
        {Y: step(y, ky), C: (other if kc else c)}
        for ky in range(4) for kc in range(2) if ky or kc
    ]
    z_peers = [{Z: step(z, k)} for k in (1, 2, 3)]

    for i, (slots, targets) in enumerate(((norm_x, x_peers), (norm_y, y_peers), (norm_z, z_peers))):
        exchange(squares, slots, targets, i)
        landed(slots, small_sem.at[i])
        pltpu.make_async_copy(slots, slots, small_send.at[i]).wait()
        squares[...] += jnp.sum(slots[...], axis=0)

    square_sum = jnp.sum(squares[...], keepdims=True)
    clip_scale = clip_limit / jnp.maximum(jnp.sqrt(square_sum), clip_limit)

    tile = 32
    first_top = jnp.zeros((8, width), jnp.float32)
    second_top = jnp.zeros((8, width), jnp.float32)

    def moment(t, tops):
        here = pl.ds(pl.multiple_of(t * tile, tile), tile)
        clipped = clip_scale * grad[here, :]
        first = first_new[here, :] + (1.0 - beta_first) * clipped
        second = second_new[here, :] + (1.0 - beta_second) * clipped * clipped
        first_new[here, :] = first
        second_new[here, :] = second
        outs = []
        for i, (value, top) in enumerate(((jnp.abs(first), tops[0]), (second, tops[1]))):
            outs.append(jnp.maximum(top, jnp.max(value.reshape(tile // 8, 8, width), axis=0)))
            most = value[:, :128]
            for j in range(1, width // 128):
                most = jnp.maximum(most, value[:, j * 128 : (j + 1) * 128])
            rowmax[i, here, :] = most
        return tuple(outs)

    first_top, second_top = lax.fori_loop(0, grad.shape[0] // tile, moment, (first_top, second_top))
    colmax[0:1, :] = jnp.max(first_top, axis=0, keepdims=True)
    colmax[1:2, :] = jnp.max(second_top, axis=0, keepdims=True)

    exchange(colmax, col_y, y_peers, 3)
    first_row = jnp.max(jnp.transpose(rowmax[0]), axis=0, keepdims=True)
    first_rowmax[...] = jnp.maximum(first_row, scale_floor)
    second_rowmax[...] = jnp.max(jnp.transpose(rowmax[1]), axis=0, keepdims=True)
    landed(col_y, small_sem.at[3])
    pltpu.make_async_copy(col_y, col_y, small_send.at[3]).wait()
    colmax[...] = jnp.maximum(colmax[...], jnp.max(col_y[...], axis=0))
    exchange(colmax, col_z, z_peers, 4)
    landed(col_z, small_sem.at[4])
    result = jnp.maximum(colmax[...], jnp.max(col_z[...], axis=0))
    first_colmax[...] = jnp.maximum(result[0:1], scale_floor)
    second_colmax[...] = result[1:2]
    pltpu.make_async_copy(col_z, col_z, small_send.at[4]).wait()

    landed(got, got_send)
    for kind, (ref, ref_t) in enumerate((
        (sent_l, sent_lt), (sent_m, sent_mt), (sent_l2, sent_l2t), (sent_m2, sent_m2t),
    )):
        landed(ref, sends.at[kind])
        landed(ref_t, sends.at[kind + 4])


def scale(
    first_new, second_new, first_rowmax, first_colmax, second_rowmax, second_colmax,
    direction, first_scaled, second_scaled, *maxima,
):
    first, second = first_new[...], second_new[...]
    direction[...] = first / (jnp.sqrt(second) + epsilon)
    rows, width = first.shape
    for value, row, col, out in (
        (first, first_rowmax, first_colmax, first_scaled),
        (second, second_rowmax, second_colmax, second_scaled),
    ):
        by_row = jnp.transpose(jnp.broadcast_to(row[...], (128, rows)))
        for j in range(width // 128):
            cols = slice(j * 128, j * 128 + 128)
            out[:, cols] = value[:, cols] / jnp.minimum(by_row, col[:, cols])
    for ref, out in zip((first_rowmax, first_colmax, second_rowmax, second_colmax), maxima):
        out[...] = ref[...]


def local(
    grad_parts, first_codes, first_rows, first_columns, second_codes, second_rows, second_columns
):
    layer_count, _, row_count, col_count = grad_parts.shape
    entries = layer_count * lax.axis_size(X) * row_count * col_count
    clip_limit = clip_rms * math.sqrt(entries)
    own_rows = first_codes.shape[1]
    rows = own_rows // SLICES
    q = col_count // 4
    f32, bf16 = jnp.float32, jnp.bfloat16
    shape = jax.ShapeDtypeStruct
    vmem = pltpu.VMEM
    dma = pltpu.SemaphoreType.DMA
    grads = grad_parts.reshape(4, 4, 2, own_rows, col_count)
    any_spec = pl.BlockSpec(memory_space=pl.ANY)
    vmem_spec = pl.BlockSpec(memory_space=pltpu.VMEM)
    n = SLICES

    def coded(count):
        return vmem((n, 2, 2, count, rows, q), jnp.int16), vmem((n, 2, 2, count, q), f32)

    first_new, second_new, first_rowmax, first_colmax, second_rowmax, second_colmax = pl.pallas_call(
        functools.partial(kernel, clip_limit),
        out_shape=(
            shape((own_rows, col_count), f32), shape((own_rows, col_count), f32),
            shape((1, own_rows), f32), shape((1, col_count), f32),
            shape((1, own_rows), f32), shape((1, col_count), f32),
        ),
        in_specs=[any_spec, any_spec, vmem_spec, vmem_spec, any_spec, vmem_spec, vmem_spec],
        out_specs=[vmem_spec] * 6,
        scratch_shapes=[
            vmem((n, 4, 4, rows, col_count), bf16),
            vmem((n, 4, 4, rows, col_count), bf16),
            *coded(8), *coded(8),
            *coded(4), *coded(4),
            vmem((n, 2, 2, 4, rows, q), f32),
            *coded(2), *coded(2),
            *coded(1), *coded(1),
            vmem((2, own_rows, col_count), jnp.int32),
            vmem((own_rows, col_count), f32),
            vmem((8, 128), f32),
            vmem((3, 8, 128), f32),
            vmem((7, 8, 128), f32),
            vmem((3, 8, 128), f32),
            vmem((2, own_rows, 128), f32),
            vmem((2, col_count), f32),
            vmem((7, 2, col_count), f32),
            vmem((3, 2, col_count), f32),
            dma((n,)), dma((n,)), dma((2,)),
            *[dma((n, 2, 2, 2))] * 4, dma((5,)),
            dma, dma((8,)), dma((5,)),
        ],
        compiler_params=pltpu.CompilerParams(
            collective_id=0, has_side_effects=True, vmem_limit_bytes=67043328
        ),
        name="clipped_adam",
    )(
        grads, first_codes[0], first_rows, first_columns, second_codes[0], second_rows,
        second_columns,
    )
    part = own_rows // 2
    tile = pl.BlockSpec((part, col_count), lambda i: (i, 0))
    row = pl.BlockSpec((1, part), lambda i: (0, i))
    column = pl.BlockSpec((1, col_count), lambda i: (0, 0))
    big, by_row, by_col = (shape(s, f32) for s in ((own_rows, col_count), (1, own_rows), (1, col_count)))
    direction, first_scaled, second_scaled, *maxima = pl.pallas_call(
        scale,
        grid=(own_rows // part,),
        out_shape=(big, big, big, by_row, by_col, by_row, by_col),
        in_specs=[tile, tile, row, column, row, column],
        out_specs=[tile, tile, tile, row, column, row, column],
        name="scale",
    )(first_new, second_new, first_rowmax, first_colmax, second_rowmax, second_colmax)
    return direction[None], first_scaled[None], second_scaled[None], *maxima


def solution(mesh):
    torus = Mesh(mesh.devices.reshape(mesh.shape["section"], 4, 4, 2), (X, Y, Z, C))
    placed = (
        P(X, FSDP, None, None),
        P(X, FSDP, None),
        P(X, FSDP),
        P(X, None),
        P(X, FSDP, None),
        P(X, FSDP),
        P(X, None),
    )
    return jax.shard_map(
        local,
        mesh=torus,
        in_specs=placed,
        out_specs=(
            P(X, FSDP, None), P(X, FSDP, None), P(X, FSDP, None),
            P(X, FSDP), P(X, None), P(X, FSDP), P(X, None),
        ),
        check_vma=False,
    )
```

```python
import functools
import math

import jax
import jax.numpy as jnp
from jax import lax
from jax.experimental import pallas as pl
from jax.experimental.pallas import tpu as pltpu
from jax.sharding import Mesh
from jax.sharding import PartitionSpec as P

Y, Z, C, X = "fsdp_0", "fsdp_1", "fsdp_2", "section"
FSDP = (Y, Z, C)
MESH = pl.DeviceIdType.MESH

beta_first = 0.9
beta_second = 0.999
clip_rms = 3.0
epsilon = 1e-08
scale_floor = 0.001

SLICES = 8
AHEAD = 3
TILES = 8
LEVELS = 32766.0
TINY = 2e-34
DIRS = ((0, 1), (1, 3))


def remote(src, dst, send, recv, device):
    return pltpu.make_async_remote_copy(
        src_ref=src, dst_ref=dst, send_sem=send, recv_sem=recv,
        device_id=device, device_id_type=MESH,
    )


def landed(buf, sem):
    pltpu.make_async_copy(buf, buf, sem).wait()


def put(values, codes, tops, key):
    rows = []
    for i, value in enumerate(values):
        top = jnp.maximum(jnp.max(jnp.abs(value), axis=0, keepdims=True), TINY) * 1.008
        top = top.astype(jnp.bfloat16).astype(jnp.float32)
        scaled = jnp.round(value * (LEVELS / top))
        codes[(*key, i)] = scaled.astype(jnp.int32).astype(jnp.int16)
        rows.append(top)
    tops[key] = jnp.concatenate(rows, axis=0).astype(tops.dtype)


def take(codes, tops, key, i):
    unit = tops[key].astype(jnp.float32)[i : i + 1] * (1.0 / LEVELS)
    return codes[(*key, i)].astype(jnp.int32).astype(jnp.float32) * unit


def kernel(
    clip_limit,
    grads, first_codes, first_rows, first_columns, second_codes, second_rows, second_columns,
    first_new, second_new, first_rowmax, first_colmax, second_rowmax, second_colmax,
    own, got, sent_l, sent_lt, came_l, came_lt, sent_m, sent_mt, came_m, came_mt, total,
    sent_l2, sent_l2t, came_l2, came_l2t, sent_m2, sent_m2t, came_m2, came_m2t,
    codes, grad, sums, squares, norm_x, norm_p, rowmax, colmax, col_y, col_z,
    first_r, first_c, second_r, second_c, words_ref, gift,
    own_sem, got_sem, code_sem, l_sem, m_sem, l2_sem, m2_sem, small_sem,
    got_send, sends, small_send,
):
    slices, _, _, rows, width = own.shape
    quarter = width // 4
    y, z, c, x = (lax.axis_index(a) for a in (Y, Z, C, X))
    at = (y, z)
    names = (Y, Z)
    other = 1 - c

    def step(v, k):
        return lax.rem(v + k, 4)

    half = pltpu.make_async_copy(grads.at[:, :, other, pl.ds(0, rows), :], gift, own_sem.at[2])
    half.start()

    def load(p, sem):
        pltpu.make_async_copy(
            grads.at[:, :, c, pl.ds(p * rows, rows), :], own.at[p], own_sem.at[sem]
        ).start()
        return sem

    load(0, 0)
    lax.fori_loop(1, slices, load, 1)
    small = (
        (first_rows, first_r), (first_columns, first_c), (second_rows, second_r),
        (second_columns, second_c),
    )
    for i, (ref, to) in enumerate((
        (first_codes, codes.at[0]), (second_codes, codes.at[1]), *small,
    )):
        pltpu.make_async_copy(ref, to, code_sem.at[0 if i < 2 else 1]).start()

    barrier = pltpu.get_barrier_semaphore()
    peers = [{C: other}]
    for axis, name in enumerate(names):
        for k in (1, 3):
            peers.append({name: step(at[axis], k)})
    for k in (1, 2, 3):
        peers.append({X: step(x, k)})
    for peer in peers:
        pl.semaphore_signal(barrier, inc=1, device_id=peer, device_id_type=MESH)
    pl.semaphore_wait(barrier, len(peers))

    def give(p, _):
        remote(
            grads.at[:, :, other, pl.ds(p * rows, rows), :], got.at[p],
            got_send, got_sem.at[p], {C: other},
        ).start()
        return _

    halves = [pl.ds(0, 2 * quarter), pl.ds(2 * quarter, 2 * quarter)]
    half.wait()
    for axis in (0, 1):
        remote(
            gift.at[:, :, :, halves[axis]], got.at[0, :, :, :, halves[axis]],
            got_send, got_sem.at[axis * slices], {C: other},
        ).start()
    lax.fori_loop(1, AHEAD + 1, give, 0)

    def columns(axis, slot):
        return pl.ds((2 * axis + slot) * quarter, quarter)

    def pair(p, axis, index, j, slot):
        where = (p, index, j) if axis == 0 else (p, j, index)
        where = (*where, slice(None), columns(axis, slot))
        return own[where].astype(jnp.float32) + got[where].astype(jnp.float32)

    def send(kind, key, ref, ref_t, out, out_t, sem, device):
        remote(ref.at[key], out.at[key], sends.at[kind], sem, device).start()
        remote(ref_t.at[key], out_t.at[key], sends.at[kind + 4], sem, device).start()

    def arrived(messages, slabs, sem):
        words = messages * (slabs * rows * quarter // 2 + max(slabs, 2) * quarter // 2)
        landed(words_ref.at[:, pl.ds(0, words)], sem)

    def leaves(p, ready):
        @pl.when(p + AHEAD + 1 < slices)
        def _next():
            give(p + AHEAD + 1, 0)

        for axis in (0, 1):
            me = at[axis]
            ready(axis)
            for slot, k in DIRS:
                values = [pair(p, axis, step(me, 2), j, slot) for j in range(4)]
                values += [pair(p, axis, step(me, k), j, 1 - slot) for j in range(4)]
                put(values, sent_l, sent_lt, (p, axis, slot))
                send(0, (p, axis, slot), sent_l, sent_lt, came_l, came_lt, l_sem.at[p],
                     {names[axis]: step(me, k)})

    def first_ready(axis):
        if axis == 0:
            landed(own.at[0], own_sem.at[0])
        landed(got.at[0, :, :, :, halves[axis]], got_sem.at[axis * slices])

    def later(p, _):
        leaves(p, lambda axis: None if axis else landed(got.at[p], got_sem.at[p]))
        return _

    leaves(0, first_ready)
    landed(own.at[pl.ds(1, slices - 1)], own_sem.at[1])
    lax.fori_loop(1, AHEAD, later, 0)

    def middles(p, _):
        arrived(4, 8, l_sem.at[p])
        for axis in (0, 1):
            me = at[axis]
            for slot, k in DIRS:
                key = (p, axis, slot)
                values = [
                    pair(p, axis, step(me, k), j, slot) + take(came_l, came_lt, key, j)
                    for j in range(4)
                ]
                put(values, sent_m, sent_mt, key)
                send(1, key, sent_m, sent_mt, came_m, came_mt, m_sem.at[p],
                     {names[axis]: step(me, k)})
        return _

    def both(p, _):
        @pl.when(p + AHEAD < slices)
        def _next():
            later(p + AHEAD, 0)

        return middles(p, _)

    lax.fori_loop(0, slices, both, 0)

    landed(codes, code_sem.at[0])
    landed(words_ref.at[:, pl.ds(0, 2 * (grad.shape[0] + width))], code_sem.at[1])
    for i, (row_ref, col_ref, out, factor) in enumerate((
        (first_r, first_c, first_new, beta_first / 7.0),
        (second_r, second_c, second_new, beta_second / 15.0),
    )):
        row_count = row_ref.shape[1]
        by_row = jnp.transpose(jnp.broadcast_to(row_ref[...], (128, row_count)))
        for j in range(width // 128):
            cols = pl.ds(j * 128, 128)
            bound = jnp.minimum(by_row, col_ref[:, cols])
            out[:, cols] = codes[i, :, cols].astype(jnp.float32) * factor * bound

    def totals(p, _):
        arrived(4, 4, m_sem.at[p])
        for axis in (0, 1):
            me, over, across = at[axis], at[1 - axis], names[1 - axis]
            for slot, k in DIRS:
                for j in range(4):
                    total[p, axis, slot, j] = (
                        pair(p, axis, me, j, slot)
                        + take(came_m, came_mt, (p, axis, slot), j)
                        + take(came_l, came_lt, (p, axis, 1 - slot), 4 + j)
                    )
            for slot, k in DIRS:
                values = [
                    total[p, axis, which, step(over, index)]
                    for which, index in ((slot, 2), (1 - slot, k))
                ]
                put(values, sent_l2, sent_l2t, (p, axis, slot))
                send(2, (p, axis, slot), sent_l2, sent_l2t, came_l2, came_l2t, l2_sem.at[p],
                     {across: step(over, k)})
        return _

    lax.fori_loop(0, slices, totals, 0)

    def middles2(p, _):
        arrived(4, 2, l2_sem.at[p])
        for axis in (0, 1):
            over, across = at[1 - axis], names[1 - axis]
            for slot, k in DIRS:
                key = (p, axis, slot)
                value = total[p, axis, slot, step(over, k)] + take(came_l2, came_l2t, key, 0)
                put([value], sent_m2, sent_m2t, key)
                send(3, key, sent_m2, sent_m2t, came_m2, came_m2t, m2_sem.at[p],
                     {across: step(over, k)})
        return _

    lax.fori_loop(0, slices, middles2, 0)

    sums[...] = jnp.zeros_like(sums)

    def finish(p, _):
        arrived(4, 1, m2_sem.at[p])
        for axis in (0, 1):
            over = at[1 - axis]
            for slot, k in DIRS:
                value = (
                    total[p, axis, slot, over]
                    + take(came_m2, came_m2t, (p, axis, slot), 0)
                    + take(came_l2, came_l2t, (p, axis, 1 - slot), 1)
                )
                grad[pl.ds(pl.multiple_of(p * rows, rows), rows), columns(axis, slot)] = value
                sq = value * value
                part = sq[:, :128]
                for j in range(1, quarter // 128):
                    part = part + sq[:, j * 128 : (j + 1) * 128]
                sums[...] += jnp.sum(part.reshape(rows // 8, 8, 128), axis=0)
        return _

    lax.fori_loop(0, slices, finish, 0)
    squares[...] = jnp.sum(sums[...], axis=0, keepdims=True)

    def exchange(value_ref, slots, targets, sem):
        for i, target in enumerate(targets):
            remote(value_ref, slots.at[i], small_send.at[sem], small_sem.at[sem], target).start()

    x_peers = [{X: step(x, k)} for k in (1, 2, 3)]
    y_peers = [
        {Y: step(y, ky), C: (other if kc else c)}
        for ky in range(4) for kc in range(2) if ky or kc
    ]
    z_peers = [{Z: step(z, k)} for k in (1, 2, 3)]
    all_peers = [
        {Y: step(y, ky), Z: step(z, kz), C: (other if kc else c)}
        for ky in range(4) for kz in range(4) for kc in range(2) if ky or kz or kc
    ]

    for i, (slots, targets) in enumerate(((norm_x, x_peers), (norm_p, all_peers))):
        exchange(squares, slots, targets, i)
        landed(slots, small_sem.at[i])
        pltpu.make_async_copy(slots, slots, small_send.at[i]).wait()
        squares[...] += jnp.sum(slots[...], axis=0)

    square_sum = jnp.sum(squares[...], keepdims=True)
    clip_scale = clip_limit / jnp.maximum(jnp.sqrt(square_sum), clip_limit)

    tile = 32
    first_top = jnp.zeros((8, width), jnp.float32)
    second_top = jnp.zeros((8, width), jnp.float32)

    def moment(t, tops):
        here = pl.ds(pl.multiple_of(t * tile, tile), tile)
        clipped = clip_scale * grad[here, :]
        first = first_new[here, :] + (1.0 - beta_first) * clipped
        second = second_new[here, :] + (1.0 - beta_second) * clipped * clipped
        first_new[here, :] = first
        second_new[here, :] = second
        outs = []
        for i, (value, top) in enumerate(((jnp.abs(first), tops[0]), (second, tops[1]))):
            outs.append(jnp.maximum(top, jnp.max(value.reshape(tile // 8, 8, width), axis=0)))
            most = value[:, :128]
            for j in range(1, width // 128):
                most = jnp.maximum(most, value[:, j * 128 : (j + 1) * 128])
            rowmax[i, here, :] = most
        return tuple(outs)

    first_top, second_top = lax.fori_loop(0, grad.shape[0] // tile, moment, (first_top, second_top))
    colmax[0:1, :] = jnp.max(first_top, axis=0, keepdims=True)
    colmax[1:2, :] = jnp.max(second_top, axis=0, keepdims=True)

    exchange(colmax, col_y, y_peers, 2)
    first_row = jnp.max(jnp.transpose(rowmax[0]), axis=0, keepdims=True)
    first_rowmax[...] = jnp.maximum(first_row, scale_floor)
    second_rowmax[...] = jnp.max(jnp.transpose(rowmax[1]), axis=0, keepdims=True)

    landed(col_y, small_sem.at[2])
    pltpu.make_async_copy(col_y, col_y, small_send.at[2]).wait()
    colmax[...] = jnp.maximum(colmax[...], jnp.max(col_y[...], axis=0))
    exchange(colmax, col_z, z_peers, 3)
    landed(col_z, small_sem.at[3])
    result = jnp.maximum(colmax[...], jnp.max(col_z[...], axis=0))
    first_colmax[...] = jnp.maximum(result[0:1], scale_floor)
    second_colmax[...] = result[1:2]
    pltpu.make_async_copy(col_z, col_z, small_send.at[3]).wait()

    landed(got, got_send)
    for kind, (ref, ref_t) in enumerate((
        (sent_l, sent_lt), (sent_m, sent_mt), (sent_l2, sent_l2t), (sent_m2, sent_m2t),
    )):
        landed(ref, sends.at[kind])
        landed(ref_t, sends.at[kind + 4])


def scale(
    first_new, second_new, first_rowmax, first_colmax, second_rowmax, second_colmax,
    direction, first_scaled, second_scaled,
    first_row_out, first_col_out, second_row_out, second_col_out,
    out, out_sem, max_sem,
):
    copies = [
        pltpu.make_async_copy(ref, to, max_sem.at[i]) for i, (ref, to) in enumerate((
            (first_rowmax, first_row_out), (first_colmax, first_col_out),
            (second_rowmax, second_row_out), (second_colmax, second_col_out),
        ))
    ]
    for copy in copies:
        copy.start()
    rows, width = first_new.shape
    tile = rows // TILES
    by_row = [
        jnp.transpose(jnp.broadcast_to(ref[...], (128, rows)))
        for ref in (first_rowmax, second_rowmax)
    ]
    for t in range(TILES):
        here = slice(t * tile, (t + 1) * tile)
        for j in range(width // 128):
            cols = slice(j * 128, j * 128 + 128)
            first, second = first_new[here, cols], second_new[here, cols]
            out[0, here, cols] = first / (jnp.sqrt(second) + epsilon)
            out[1, here, cols] = first / jnp.minimum(by_row[0][here], first_colmax[:, cols])
            out[2, here, cols] = second / jnp.minimum(by_row[1][here], second_colmax[:, cols])
        for i, to in enumerate((direction, first_scaled, second_scaled)):
            copy = pltpu.make_async_copy(out.at[i, here], to.at[here], out_sem.at[t, i])
            copy.start()
            copies.append(copy)
    for copy in copies:
        copy.wait()


def local(
    grad_parts, first_codes, first_rows, first_columns, second_codes, second_rows, second_columns
):
    layer_count, _, row_count, col_count = grad_parts.shape
    entries = layer_count * lax.axis_size(X) * row_count * col_count
    clip_limit = clip_rms * math.sqrt(entries)
    own_rows = first_codes.shape[1]
    rows = own_rows // SLICES
    q = col_count // 4
    f32, bf16 = jnp.float32, jnp.bfloat16
    shape = jax.ShapeDtypeStruct
    vmem = pltpu.VMEM
    dma = pltpu.SemaphoreType.DMA
    grads = grad_parts.reshape(4, 4, 2, own_rows, col_count)
    hbm_spec = pl.BlockSpec(memory_space=pltpu.HBM)
    vmem_spec = pl.BlockSpec(memory_space=pltpu.VMEM)
    n = SLICES

    def coded(count):
        return vmem((n, 2, 2, count, rows, q), jnp.int16), vmem((n, 2, 2, count, q), bf16 if count > 1 else f32)

    first_new, second_new, first_rowmax, first_colmax, second_rowmax, second_colmax = pl.pallas_call(
        functools.partial(kernel, clip_limit),
        out_shape=(
            shape((own_rows, col_count), f32), shape((own_rows, col_count), f32),
            shape((1, own_rows), f32), shape((1, col_count), f32),
            shape((1, own_rows), f32), shape((1, col_count), f32),
        ),
        in_specs=[hbm_spec] * 7,
        out_specs=[vmem_spec] * 6,
        scratch_shapes=[
            vmem((n, 4, 4, rows, col_count), bf16),
            vmem((n, 4, 4, rows, col_count), bf16),
            *coded(8), *coded(8),
            *coded(4), *coded(4),
            vmem((n, 2, 2, 4, rows, q), f32),
            *coded(2), *coded(2),
            *coded(1), *coded(1),
            vmem((2, own_rows, col_count), jnp.int32),
            vmem((own_rows, col_count), f32),
            vmem((8, 128), f32),
            vmem((1, 128), f32),
            vmem((3, 1, 128), f32),
            vmem((31, 1, 128), f32),
            vmem((2, own_rows, 128), f32),
            vmem((2, col_count), f32),
            vmem((7, 2, col_count), f32),
            vmem((3, 2, col_count), f32),
            *[vmem((1, own_rows), f32), vmem((1, col_count), f32)] * 2,
            vmem((1, 16 * (rows + 1) * q), f32),
            vmem((4, 4, rows, col_count), bf16),
            dma((3,)), dma((n + 1,)), dma((2,)),
            dma((n,)), dma((n,)), dma((n,)), dma((n,)), dma((4,)),
            dma, dma((8,)), dma((4,)),
        ],
        compiler_params=pltpu.CompilerParams(
            collective_id=0, has_side_effects=True, vmem_limit_bytes=46 * 2**20
        ),
        name="clipped_adam",
    )(
        *(
            pltpu.with_memory_space_constraint(v, pltpu.HBM)
            for v in (
                grads, first_codes[0], first_rows, first_columns, second_codes[0], second_rows,
                second_columns,
            )
        )
    )
    big, by_row, by_col = (shape(s, f32) for s in ((own_rows, col_count), (1, own_rows), (1, col_count)))
    direction, first_scaled, second_scaled, *maxima = pl.pallas_call(
        scale,
        out_shape=(big, big, big, by_row, by_col, by_row, by_col),
        in_specs=[vmem_spec] * 6,
        out_specs=[hbm_spec] * 7,
        scratch_shapes=[vmem((3, own_rows, col_count), f32), dma((TILES, 3)), dma((4,))],
        compiler_params=pltpu.CompilerParams(vmem_limit_bytes=12 * 2**20),
        name="scale",
    )(first_new, second_new, first_rowmax, first_colmax, second_rowmax, second_colmax)
    return direction[None], first_scaled[None], second_scaled[None], *maxima


def solution(mesh):
    torus = Mesh(mesh.devices.reshape(mesh.shape["section"], 4, 4, 2), (X, Y, Z, C))
    placed = (
        P(X, FSDP, None, None),
        P(X, FSDP, None),
        P(X, FSDP),
        P(X, None),
        P(X, FSDP, None),
        P(X, FSDP),
        P(X, None),
    )
    return jax.shard_map(
        local,
        mesh=torus,
        in_specs=placed,
        out_specs=(
            P(X, FSDP, None), P(X, FSDP, None), P(X, FSDP, None),
            P(X, FSDP), P(X, None), P(X, FSDP), P(X, None),
        ),
        check_vma=False,
    )
```

```python
import functools
import math

import jax
import jax.numpy as jnp
from jax import lax
from jax.experimental import pallas as pl
from jax.experimental.pallas import tpu as pltpu
from jax.sharding import Mesh
from jax.sharding import PartitionSpec as P

Y, Z, C, X = "fsdp_0", "fsdp_1", "fsdp_2", "section"
FSDP = (Y, Z, C)
MESH = pl.DeviceIdType.MESH

beta_first = 0.9
beta_second = 0.999
clip_rms = 3.0
epsilon = 1e-08
scale_floor = 0.001

SLICES = 8
AHEAD = 3
ROUNDS = 6
TILES = 8
LEVELS = 32766.0
TINY = 2e-34
DIRS = ((0, 1), (1, 3))


def remote(src, dst, send, recv, device):
    return pltpu.make_async_remote_copy(
        src_ref=src, dst_ref=dst, send_sem=send, recv_sem=recv,
        device_id=device, device_id_type=MESH,
    )


def landed(buf, sem):
    pltpu.make_async_copy(buf, buf, sem).wait()


def put(values, codes, tops, key):
    rows = []
    for i, value in enumerate(values):
        top = jnp.maximum(jnp.max(jnp.abs(value), axis=0, keepdims=True), TINY) * 1.008
        top = top.astype(jnp.bfloat16).astype(jnp.float32)
        scaled = jnp.round(value * (LEVELS / top))
        codes[(*key, i)] = scaled.astype(jnp.int32).astype(jnp.int16)
        rows.append(top)
    tops[key] = jnp.concatenate(rows, axis=0).astype(tops.dtype)


def take(codes, tops, key, i):
    unit = tops[key].astype(jnp.float32)[i : i + 1] * (1.0 / LEVELS)
    return codes[(*key, i)].astype(jnp.int32).astype(jnp.float32) * unit


def kernel(
    clip_limit,
    grads, first_codes, first_rows, first_columns, second_codes, second_rows, second_columns,
    first_new, second_new, first_rowmax, first_colmax, second_rowmax, second_colmax,
    own, got, sent_l, sent_lt, came_l, came_lt, sent_m, sent_mt, came_m, came_mt, total,
    sent_l2, sent_l2t, came_l2, came_l2t, sent_m2, sent_m2t, came_m2, came_m2t,
    codes, grad, sums, squares, norm_c, norm_p, rowmax, colmax, col_c, col_z,
    first_r, first_c, second_r, second_c, words_ref, gift,
    own_sem, got_sem, code_sem, l_sem, m_sem, l2_sem, m2_sem, small_sem,
    got_send, sends, small_send, word_sem,
):
    slices, _, _, rows, width = own.shape
    quarter = width // 4
    y, z, c, x = (lax.axis_index(a) for a in (Y, Z, C, X))
    at = (y, z)
    names = (Y, Z)
    other = 1 - c

    def step(v, k):
        return lax.rem(v + k, 4)

    barrier = pltpu.get_barrier_semaphore()
    peers = [{C: other}]
    for axis, name in enumerate(names):
        for k in (1, 3):
            peers.append({name: step(at[axis], k)})
    for k in (1, 3):
        peers.append({X: step(x, k)})
    for peer in peers:
        pl.semaphore_signal(barrier, inc=1, device_id=peer, device_id_type=MESH)

    half = pltpu.make_async_copy(grads.at[:, :, other, pl.ds(0, rows), :], gift, own_sem.at[2])
    half.start()

    def load(p, sem):
        pltpu.make_async_copy(
            grads.at[:, :, c, pl.ds(p * rows, rows), :], own.at[p], own_sem.at[sem]
        ).start()
        return sem

    load(0, 0)
    lax.fori_loop(1, slices, load, 1)
    small = (
        (first_rows, first_r), (first_columns, first_c), (second_rows, second_r),
        (second_columns, second_c),
    )
    for i, (ref, to) in enumerate((
        (first_codes, codes.at[0]), (second_codes, codes.at[1]), *small,
    )):
        pltpu.make_async_copy(ref, to, code_sem.at[0 if i < 2 else 1]).start()

    pl.semaphore_wait(barrier, len(peers))
    def spread_word(p):
        @pl.when((p > 0) & (p <= ROUNDS))
        def _hear():
            pl.semaphore_wait(word_sem.at[p - 1], len(peers))

        @pl.when(p < ROUNDS)
        def _tell():
            for peer in peers:
                pl.semaphore_signal(
                    word_sem.at[p], inc=1, device_id=peer, device_id_type=MESH
                )

    def give(p, _):
        remote(
            grads.at[:, :, other, pl.ds(p * rows, rows), :], got.at[p],
            got_send, got_sem.at[p], {C: other},
        ).start()
        return _

    halves = [pl.ds(0, 2 * quarter), pl.ds(2 * quarter, 2 * quarter)]
    half.wait()
    for axis in (0, 1):
        remote(
            gift.at[:, :, :, halves[axis]], got.at[0, :, :, :, halves[axis]],
            got_send, got_sem.at[axis * slices], {C: other},
        ).start()
    lax.fori_loop(1, AHEAD + 1, give, 0)

    def columns(axis, slot):
        return pl.ds((2 * axis + slot) * quarter, quarter)

    def pair(p, axis, index, j, slot):
        where = (p, index, j) if axis == 0 else (p, j, index)
        where = (*where, slice(None), columns(axis, slot))
        return own[where].astype(jnp.float32) + got[where].astype(jnp.float32)

    def send(kind, key, ref, ref_t, out, out_t, sem, device):
        remote(ref.at[key], out.at[key], sends.at[kind], sem, device).start()
        remote(ref_t.at[key], out_t.at[key], sends.at[kind + 4], sem, device).start()

    def arrived(messages, slabs, sem):
        words = messages * (slabs * rows * quarter // 2 + max(slabs, 2) * quarter // 2)
        landed(words_ref.at[:, pl.ds(0, words)], sem)

    def leaves(p, ready):
        @pl.when(p + AHEAD + 1 < slices)
        def _next():
            give(p + AHEAD + 1, 0)

        for axis in (0, 1):
            me = at[axis]
            ready(axis)
            for slot, k in DIRS:
                values = [pair(p, axis, step(me, 2), j, slot) for j in range(4)]
                values += [pair(p, axis, step(me, k), j, 1 - slot) for j in range(4)]
                put(values, sent_l, sent_lt, (p, axis, slot))
                send(0, (p, axis, slot), sent_l, sent_lt, came_l, came_lt, l_sem.at[p],
                     {names[axis]: step(me, k)})

    def first_ready(axis):
        if axis == 0:
            landed(own.at[0], own_sem.at[0])
        landed(got.at[0, :, :, :, halves[axis]], got_sem.at[axis * slices])

    def later(p, _):
        leaves(p, lambda axis: None if axis else landed(got.at[p], got_sem.at[p]))
        return _

    leaves(0, first_ready)
    landed(own.at[pl.ds(1, slices - 1)], own_sem.at[1])
    lax.fori_loop(1, AHEAD, later, 0)

    def middles(p, _):
        arrived(4, 8, l_sem.at[p])
        for axis in (0, 1):
            me = at[axis]
            for slot, k in DIRS:
                key = (p, axis, slot)
                values = [
                    pair(p, axis, step(me, k), j, slot) + take(came_l, came_lt, key, j)
                    for j in range(4)
                ]
                put(values, sent_m, sent_mt, key)
                send(1, key, sent_m, sent_mt, came_m, came_mt, m_sem.at[p],
                     {names[axis]: step(me, k)})
        return _

    def both(p, _):
        spread_word(p)

        @pl.when(p + AHEAD < slices)
        def _next():
            later(p + AHEAD, 0)

        return middles(p, _)

    lax.fori_loop(0, slices, both, 0)

    landed(codes, code_sem.at[0])
    landed(words_ref.at[:, pl.ds(0, 2 * (grad.shape[0] + width))], code_sem.at[1])
    for i, (row_ref, col_ref, out, factor) in enumerate((
        (first_r, first_c, first_new, beta_first / 7.0),
        (second_r, second_c, second_new, beta_second / 15.0),
    )):
        row_count = row_ref.shape[1]
        by_row = jnp.transpose(jnp.broadcast_to(row_ref[...], (128, row_count)))
        for j in range(width // 128):
            cols = pl.ds(j * 128, 128)
            bound = jnp.minimum(by_row, col_ref[:, cols])
            out[:, cols] = codes[i, :, cols].astype(jnp.float32) * factor * bound

    def totals(p, _):
        arrived(4, 4, m_sem.at[p])
        for axis in (0, 1):
            me, over, across = at[axis], at[1 - axis], names[1 - axis]
            for slot, k in DIRS:
                for j in range(4):
                    total[p, axis, slot, j] = (
                        pair(p, axis, me, j, slot)
                        + take(came_m, came_mt, (p, axis, slot), j)
                        + take(came_l, came_lt, (p, axis, 1 - slot), 4 + j)
                    )
            for slot, k in DIRS:
                values = [
                    total[p, axis, which, step(over, index)]
                    for which, index in ((slot, 2), (1 - slot, k))
                ]
                put(values, sent_l2, sent_l2t, (p, axis, slot))
                send(2, (p, axis, slot), sent_l2, sent_l2t, came_l2, came_l2t, l2_sem.at[p],
                     {across: step(over, k)})
        return _

    lax.fori_loop(0, slices, totals, 0)

    def middles2(p, _):
        arrived(4, 2, l2_sem.at[p])
        for axis in (0, 1):
            over, across = at[1 - axis], names[1 - axis]
            for slot, k in DIRS:
                key = (p, axis, slot)
                value = total[p, axis, slot, step(over, k)] + take(came_l2, came_l2t, key, 0)
                put([value], sent_m2, sent_m2t, key)
                send(3, key, sent_m2, sent_m2t, came_m2, came_m2t, m2_sem.at[p],
                     {across: step(over, k)})
        return _

    lax.fori_loop(0, slices, middles2, 0)

    sums[...] = jnp.zeros_like(sums)

    def finish(p, _):
        arrived(4, 1, m2_sem.at[p])
        for axis in (0, 1):
            over = at[1 - axis]
            for slot, k in DIRS:
                value = (
                    total[p, axis, slot, over]
                    + take(came_m2, came_m2t, (p, axis, slot), 0)
                    + take(came_l2, came_l2t, (p, axis, 1 - slot), 1)
                )
                grad[pl.ds(pl.multiple_of(p * rows, rows), rows), columns(axis, slot)] = value
                sq = value * value
                part = sq[:, :128]
                for j in range(1, quarter // 128):
                    part = part + sq[:, j * 128 : (j + 1) * 128]
                sums[...] += jnp.sum(part.reshape(rows // 8, 8, 128), axis=0)
        return _

    lax.fori_loop(0, slices, finish, 0)
    squares[...] = jnp.sum(sums[...], axis=0, keepdims=True)

    def exchange(value_ref, slots, targets, sem):
        for i, target in enumerate(targets):
            remote(value_ref, slots.at[i], small_send.at[sem], small_sem.at[sem], target).start()

    def spread(value_ref, slots, places, sem):
        @pl.when(c == 1)
        def _send():
            for i, place in enumerate(places):
                for core in range(2):
                    remote(
                        value_ref, slots.at[i], small_send.at[sem], small_sem.at[sem],
                        {**place, C: core},
                    ).start()

        landed(slots, small_sem.at[sem])

    def spread_done(slots, sem):
        @pl.when(c == 1)
        def _left():
            landed(slots, small_send.at[sem])
            landed(slots, small_send.at[sem])

    hops = (0, 1, 2, 1)

    def far_first(at_x):
        places = [(kx, ky, kz) for kx in at_x for ky in range(4) for kz in range(4)]
        places = [place for place in places if any(place)]
        places.sort(key=lambda place: -sum(hops[k] for k in place))
        return [{X: step(x, kx), Y: step(y, ky), Z: step(z, kz)} for kx, ky, kz in places]

    exchange(squares, norm_c, [{C: other}], 0)
    landed(norm_c, small_sem.at[0])
    landed(norm_c, small_send.at[0])
    squares[...] += norm_c[0]
    spread(squares, norm_p, far_first(range(4)), 1)
    square_sum = jnp.sum(squares[...] + jnp.sum(norm_p[...], axis=0), keepdims=True)
    clip_scale = clip_limit / jnp.maximum(jnp.sqrt(square_sum), clip_limit)

    tile = 32
    first_top = jnp.zeros((8, width), jnp.float32)
    second_top = jnp.zeros((8, width), jnp.float32)

    def moment(t, tops):
        here = pl.ds(pl.multiple_of(t * tile, tile), tile)
        clipped = clip_scale * grad[here, :]
        first = first_new[here, :] + (1.0 - beta_first) * clipped
        second = second_new[here, :] + (1.0 - beta_second) * clipped * clipped
        first_new[here, :] = first
        second_new[here, :] = second
        outs = []
        for i, (value, top) in enumerate(((jnp.abs(first), tops[0]), (second, tops[1]))):
            outs.append(jnp.maximum(top, jnp.max(value.reshape(tile // 8, 8, width), axis=0)))
            most = value[:, :128]
            for j in range(1, width // 128):
                most = jnp.maximum(most, value[:, j * 128 : (j + 1) * 128])
            rowmax[i, here, :] = most
        return tuple(outs)

    first_top, second_top = lax.fori_loop(0, grad.shape[0] // tile, moment, (first_top, second_top))
    colmax[0:1, :] = jnp.max(first_top, axis=0, keepdims=True)
    colmax[1:2, :] = jnp.max(second_top, axis=0, keepdims=True)

    exchange(colmax, col_c, [{C: other}], 2)
    first_row = jnp.max(jnp.transpose(rowmax[0]), axis=0, keepdims=True)
    first_rowmax[...] = jnp.maximum(first_row, scale_floor)
    second_rowmax[...] = jnp.max(jnp.transpose(rowmax[1]), axis=0, keepdims=True)

    landed(col_c, small_sem.at[2])
    landed(col_c, small_send.at[2])
    colmax[...] = jnp.maximum(colmax[...], col_c[0])
    spread(colmax, col_z, far_first((0,)), 3)
    result = jnp.maximum(colmax[...], jnp.max(col_z[...], axis=0))
    first_colmax[...] = jnp.maximum(result[0:1], scale_floor)
    second_colmax[...] = result[1:2]
    spread_done(norm_p, 1)
    spread_done(col_z, 3)

    landed(got, got_send)
    for kind, (ref, ref_t) in enumerate((
        (sent_l, sent_lt), (sent_m, sent_mt), (sent_l2, sent_l2t), (sent_m2, sent_m2t),
    )):
        landed(ref, sends.at[kind])
        landed(ref_t, sends.at[kind + 4])


def scale(
    first_new, second_new, first_rowmax, first_colmax, second_rowmax, second_colmax,
    direction, first_scaled, second_scaled,
    first_row_out, first_col_out, second_row_out, second_col_out,
    out, out_sem, max_sem,
):
    copies = [
        pltpu.make_async_copy(ref, to, max_sem.at[i]) for i, (ref, to) in enumerate((
            (first_rowmax, first_row_out), (first_colmax, first_col_out),
            (second_rowmax, second_row_out), (second_colmax, second_col_out),
        ))
    ]
    for copy in copies:
        copy.start()
    rows, width = first_new.shape
    tile = rows // TILES
    by_row = [
        jnp.transpose(jnp.broadcast_to(ref[...], (128, rows)))
        for ref in (first_rowmax, second_rowmax)
    ]
    for t in range(TILES):
        here = slice(t * tile, (t + 1) * tile)
        for j in range(width // 128):
            cols = slice(j * 128, j * 128 + 128)
            first, second = first_new[here, cols], second_new[here, cols]
            out[0, here, cols] = first / (jnp.sqrt(second) + epsilon)
            out[1, here, cols] = first / jnp.minimum(by_row[0][here], first_colmax[:, cols])
            out[2, here, cols] = second / jnp.minimum(by_row[1][here], second_colmax[:, cols])
        for i, to in enumerate((direction, first_scaled, second_scaled)):
            copy = pltpu.make_async_copy(out.at[i, here], to.at[here], out_sem.at[t, i])
            copy.start()
            copies.append(copy)
    for copy in copies:
        copy.wait()


def local(
    grad_parts, first_codes, first_rows, first_columns, second_codes, second_rows, second_columns
):
    layer_count, _, row_count, col_count = grad_parts.shape
    entries = layer_count * lax.axis_size(X) * row_count * col_count
    clip_limit = clip_rms * math.sqrt(entries)
    own_rows = first_codes.shape[1]
    rows = own_rows // SLICES
    q = col_count // 4
    f32, bf16 = jnp.float32, jnp.bfloat16
    shape = jax.ShapeDtypeStruct
    vmem = pltpu.VMEM
    dma = pltpu.SemaphoreType.DMA
    grads = grad_parts.reshape(4, 4, 2, own_rows, col_count)
    hbm_spec = pl.BlockSpec(memory_space=pltpu.HBM)
    vmem_spec = pl.BlockSpec(memory_space=pltpu.VMEM)
    n = SLICES

    def coded(count):
        return vmem((n, 2, 2, count, rows, q), jnp.int16), vmem((n, 2, 2, count, q), bf16 if count > 1 else f32)

    first_new, second_new, first_rowmax, first_colmax, second_rowmax, second_colmax = pl.pallas_call(
        functools.partial(kernel, clip_limit),
        out_shape=(
            shape((own_rows, col_count), f32), shape((own_rows, col_count), f32),
            shape((1, own_rows), f32), shape((1, col_count), f32),
            shape((1, own_rows), f32), shape((1, col_count), f32),
        ),
        in_specs=[hbm_spec] * 7,
        out_specs=[vmem_spec] * 6,
        scratch_shapes=[
            vmem((n, 4, 4, rows, col_count), bf16),
            vmem((n, 4, 4, rows, col_count), bf16),
            *coded(8), *coded(8),
            *coded(4), *coded(4),
            vmem((n, 2, 2, 4, rows, q), f32),
            *coded(2), *coded(2),
            *coded(1), *coded(1),
            vmem((2, own_rows, col_count), jnp.int32),
            vmem((own_rows, col_count), f32),
            vmem((8, 128), f32),
            vmem((1, 128), f32),
            vmem((1, 1, 128), f32),
            vmem((63, 1, 128), f32),
            vmem((2, own_rows, 128), f32),
            vmem((2, col_count), f32),
            vmem((1, 2, col_count), f32),
            vmem((15, 2, col_count), f32),
            *[vmem((1, own_rows), f32), vmem((1, col_count), f32)] * 2,
            vmem((1, 16 * (rows + 1) * q), f32),
            vmem((4, 4, rows, col_count), bf16),
            dma((3,)), dma((n + 1,)), dma((2,)),
            dma((n,)), dma((n,)), dma((n,)), dma((n,)), dma((4,)),
            dma, dma((8,)), dma((4,)), pltpu.SemaphoreType.REGULAR((ROUNDS,)),
        ],
        compiler_params=pltpu.CompilerParams(
            collective_id=0, has_side_effects=True, vmem_limit_bytes=46 * 2**20
        ),
        name="clipped_adam",
    )(
        *(
            pltpu.with_memory_space_constraint(v, pltpu.HBM)
            for v in (
                grads, first_codes[0], first_rows, first_columns, second_codes[0], second_rows,
                second_columns,
            )
        )
    )
    big, by_row, by_col = (shape(s, f32) for s in ((own_rows, col_count), (1, own_rows), (1, col_count)))
    direction, first_scaled, second_scaled, *maxima = pl.pallas_call(
        scale,
        out_shape=(big, big, big, by_row, by_col, by_row, by_col),
        in_specs=[vmem_spec] * 6,
        out_specs=[hbm_spec] * 7,
        scratch_shapes=[vmem((3, own_rows, col_count), f32), dma((TILES, 3)), dma((4,))],
        compiler_params=pltpu.CompilerParams(vmem_limit_bytes=12 * 2**20),
        name="scale",
    )(first_new, second_new, first_rowmax, first_colmax, second_rowmax, second_colmax)
    return direction[None], first_scaled[None], second_scaled[None], *maxima


def solution(mesh):
    torus = Mesh(mesh.devices.reshape(mesh.shape["section"], 4, 4, 2), (X, Y, Z, C))
    placed = (
        P(X, FSDP, None, None),
        P(X, FSDP, None),
        P(X, FSDP),
        P(X, None),
        P(X, FSDP, None),
        P(X, FSDP),
        P(X, None),
    )
    return jax.shard_map(
        local,
        mesh=torus,
        in_specs=placed,
        out_specs=(
            P(X, FSDP, None), P(X, FSDP, None), P(X, FSDP, None),
            P(X, FSDP), P(X, None), P(X, FSDP), P(X, None),
        ),
        check_vma=False,
    )
```

```python
import functools
import math

import jax
import jax.numpy as jnp
from jax import lax
from jax.experimental import pallas as pl
from jax.experimental.pallas import tpu as pltpu
from jax.sharding import Mesh
from jax.sharding import PartitionSpec as P

Y, Z, C, X = "fsdp_0", "fsdp_1", "fsdp_2", "section"
FSDP = (Y, Z, C)
MESH = pl.DeviceIdType.MESH

beta_first = 0.9
beta_second = 0.999
clip_rms = 3.0
epsilon = 1e-08
scale_floor = 0.001

SLICES = 8
ACROSS = 2
AHEAD = 3
ROUNDS = 6
TILES = 8
LEVELS = 32766.0
TINY = 2e-34
DIRS = ((0, 1), (1, 3))


def remote(src, dst, send, recv, device):
    return pltpu.make_async_remote_copy(
        src_ref=src, dst_ref=dst, send_sem=send, recv_sem=recv,
        device_id=device, device_id_type=MESH,
    )


def landed(buf, sem):
    pltpu.make_async_copy(buf, buf, sem).wait()


def put(values, codes, tops, key):
    rows = []
    for i, value in enumerate(values):
        top = jnp.maximum(jnp.max(jnp.abs(value), axis=0, keepdims=True), TINY) * 1.008
        top = top.astype(jnp.bfloat16).astype(jnp.float32)
        scaled = jnp.round(value * (LEVELS / top))
        codes[(*key, i)] = scaled.astype(jnp.int32).astype(jnp.int16)
        rows.append(top)
    tops[key] = jnp.concatenate(rows, axis=0).astype(tops.dtype)


def take(codes, tops, key, i):
    unit = tops[key].astype(jnp.float32)[i : i + 1] * (1.0 / LEVELS)
    return codes[(*key, i)].astype(jnp.int32).astype(jnp.float32) * unit


def kernel(
    clip_limit,
    grads, first_codes, first_rows, first_columns, second_codes, second_rows, second_columns,
    first_new, second_new, first_rowmax, first_colmax, second_rowmax, second_colmax,
    own, got, sent_l, sent_lt, came_l, came_lt, sent_m, sent_mt, came_m, came_mt, total,
    sent_l2, sent_l2t, came_l2, came_l2t, sent_m2, sent_m2t, came_m2, came_m2t,
    codes, grad, sums, squares, norm_c, norm_p, rowmax, colmax, col_c, col_z,
    first_r, first_c, second_r, second_c, words_ref, gift,
    own_sem, got_sem, code_sem, l_sem, m_sem, l2_sem, m2_sem, small_sem,
    got_send, sends, small_send, word_sem,
):
    slices, *_, rows, span = own.shape
    width = grad.shape[1]
    across = width // span
    quarter = span // 4
    y, z, c, x = (lax.axis_index(a) for a in (Y, Z, C, X))
    at = (y, z)
    names = (Y, Z)
    other = 1 - c

    def step(v, k):
        return lax.rem(v + k, 4)

    barrier = pltpu.get_barrier_semaphore()
    peers = [{C: other}]
    for axis, name in enumerate(names):
        for k in (1, 3):
            peers.append({name: step(at[axis], k), C: other})
    for k in (1, 3):
        peers.append({X: step(x, k)})
    for peer in peers:
        pl.semaphore_signal(barrier, inc=1, device_id=peer, device_id_type=MESH)

    def block(p):
        down = pl.ds(pl.multiple_of(p // across * rows, rows), rows)
        return down, pl.ds(pl.multiple_of(p % across * span, span), span)

    def pieces(p, core):
        for i in range(2):
            for j in range(2):
                whose = lax.rem(core + y + z + i + j, 2)
                yield grads.at[:, i, :, j, whose, *block(p)], (slice(None), i, slice(None), j)

    for piece, where in pieces(0, other):
        pltpu.make_async_copy(piece, gift.at[where], own_sem.at[2]).start()

    def load(p, sem):
        for piece, where in pieces(p, c):
            pltpu.make_async_copy(piece, own.at[(p, *where)], own_sem.at[sem]).start()
        return sem

    load(0, 0)
    lax.fori_loop(1, slices, load, 1)
    small = (
        (first_rows, first_r), (first_columns, first_c), (second_rows, second_r),
        (second_columns, second_c),
    )
    for i, (ref, to) in enumerate((
        (first_codes, codes.at[0]), (second_codes, codes.at[1]), *small,
    )):
        pltpu.make_async_copy(ref, to, code_sem.at[0 if i < 2 else 1]).start()

    pl.semaphore_wait(barrier, len(peers))
    def spread_word(p):
        @pl.when((p > 0) & (p <= ROUNDS))
        def _hear():
            pl.semaphore_wait(word_sem.at[p - 1], len(peers))

        @pl.when(p < ROUNDS)
        def _tell():
            for peer in peers:
                pl.semaphore_signal(
                    word_sem.at[p], inc=1, device_id=peer, device_id_type=MESH
                )

    def give(p, _):
        for piece, where in pieces(p, other):
            remote(piece, got.at[(p, *where)], got_send, got_sem.at[p], {C: other}).start()
        return _

    halves = [pl.ds(0, 2 * quarter), pl.ds(2 * quarter, 2 * quarter)]
    landed(gift, own_sem.at[2])
    for axis in (0, 1):
        remote(
            gift.at[:, :, :, :, :, halves[axis]], got.at[0, :, :, :, :, :, halves[axis]],
            got_send, got_sem.at[axis * slices], {C: other},
        ).start()
    lax.fori_loop(1, AHEAD + 1, give, 0)

    def columns(axis, slot):
        return pl.ds((2 * axis + slot) * quarter, quarter)

    def pair(p, axis, index, j, slot):
        index, j = (index // 2, index % 2), (j // 2, j % 2)
        where = (*index, *j) if axis == 0 else (*j, *index)
        where = (p, *where, slice(None), columns(axis, slot))
        return own[where].astype(jnp.float32) + got[where].astype(jnp.float32)

    def send(kind, key, ref, ref_t, out, out_t, sem, device):
        remote(ref.at[key], out.at[key], sends.at[kind], sem, device).start()
        remote(ref_t.at[key], out_t.at[key], sends.at[kind + 4], sem, device).start()

    def arrived(messages, slabs, sem):
        words = messages * (slabs * rows * quarter // 2 + max(slabs, 2) * quarter // 2)
        landed(words_ref.at[:, pl.ds(0, words)], sem)

    def leaves(p, ready):
        @pl.when(p + AHEAD + 1 < slices)
        def _next():
            give(p + AHEAD + 1, 0)

        for axis in (0, 1):
            me = at[axis]
            ready(axis)
            for slot, k in DIRS:
                values = [pair(p, axis, step(me, 2), j, slot) for j in range(4)]
                values += [pair(p, axis, step(me, k), j, 1 - slot) for j in range(4)]
                put(values, sent_l, sent_lt, (p, axis, slot))
                send(0, (p, axis, slot), sent_l, sent_lt, came_l, came_lt, l_sem.at[p],
                     {names[axis]: step(me, k), C: other})

    def first_ready(axis):
        if axis == 0:
            landed(own.at[0], own_sem.at[0])
        landed(got.at[0, :, :, :, :, :, halves[axis]], got_sem.at[axis * slices])

    def later(p, _):
        leaves(p, lambda axis: None if axis else landed(got.at[p], got_sem.at[p]))
        return _

    leaves(0, first_ready)
    landed(own.at[pl.ds(1, slices - 1)], own_sem.at[1])
    lax.fori_loop(1, AHEAD, later, 0)

    def middles(p, _):
        arrived(4, 8, l_sem.at[p])
        for axis in (0, 1):
            me = at[axis]
            for slot, k in DIRS:
                key = (p, axis, slot)
                values = [
                    pair(p, axis, step(me, k), j, slot) + take(came_l, came_lt, key, j)
                    for j in range(4)
                ]
                put(values, sent_m, sent_mt, key)
                send(1, key, sent_m, sent_mt, came_m, came_mt, m_sem.at[p],
                     {names[axis]: step(me, k), C: other})
        return _

    def both(p, _):
        spread_word(p)

        @pl.when(p + AHEAD < slices)
        def _next():
            later(p + AHEAD, 0)

        return middles(p, _)

    lax.fori_loop(0, slices, both, 0)

    landed(codes, code_sem.at[0])
    landed(words_ref.at[:, pl.ds(0, 2 * (grad.shape[0] + width))], code_sem.at[1])
    for i, (row_ref, col_ref, out, factor) in enumerate((
        (first_r, first_c, first_new, beta_first / 7.0),
        (second_r, second_c, second_new, beta_second / 15.0),
    )):
        row_count = row_ref.shape[1]
        by_row = jnp.transpose(jnp.broadcast_to(row_ref[...], (128, row_count)))
        for j in range(width // 128):
            cols = pl.ds(j * 128, 128)
            bound = jnp.minimum(by_row, col_ref[:, cols])
            out[:, cols] = codes[i, :, cols].astype(jnp.float32) * factor * bound

    def totals(p, _):
        arrived(4, 4, m_sem.at[p])
        for axis in (0, 1):
            me, over, way = at[axis], at[1 - axis], names[1 - axis]
            for slot, k in DIRS:
                for j in range(4):
                    total[p, axis, slot, j] = (
                        pair(p, axis, me, j, slot)
                        + take(came_m, came_mt, (p, axis, slot), j)
                        + take(came_l, came_lt, (p, axis, 1 - slot), 4 + j)
                    )
            for slot, k in DIRS:
                values = [
                    total[p, axis, which, step(over, index)]
                    for which, index in ((slot, 2), (1 - slot, k))
                ]
                put(values, sent_l2, sent_l2t, (p, axis, slot))
                send(2, (p, axis, slot), sent_l2, sent_l2t, came_l2, came_l2t, l2_sem.at[p],
                     {way: step(over, k), C: other})
        return _

    lax.fori_loop(0, slices, totals, 0)

    def middles2(p, _):
        arrived(4, 2, l2_sem.at[p])
        for axis in (0, 1):
            over, way = at[1 - axis], names[1 - axis]
            for slot, k in DIRS:
                key = (p, axis, slot)
                value = total[p, axis, slot, step(over, k)] + take(came_l2, came_l2t, key, 0)
                put([value], sent_m2, sent_m2t, key)
                send(3, key, sent_m2, sent_m2t, came_m2, came_m2t, m2_sem.at[p],
                     {way: step(over, k), C: other})
        return _

    lax.fori_loop(0, slices, middles2, 0)

    sums[...] = jnp.zeros_like(sums)

    def finish(p, _):
        arrived(4, 1, m2_sem.at[p])
        for axis in (0, 1):
            over = at[1 - axis]
            for slot, k in DIRS:
                value = (
                    total[p, axis, slot, over]
                    + take(came_m2, came_m2t, (p, axis, slot), 0)
                    + take(came_l2, came_l2t, (p, axis, 1 - slot), 1)
                )
                here = pl.multiple_of(p % across * span + (2 * axis + slot) * quarter, quarter)
                grad[block(p)[0], pl.ds(here, quarter)] = value
                sq = value * value
                part = sq[:, :128]
                for j in range(1, quarter // 128):
                    part = part + sq[:, j * 128 : (j + 1) * 128]
                sums[...] += jnp.sum(part.reshape(rows // 8, 8, 128), axis=0)
        return _

    lax.fori_loop(0, slices, finish, 0)
    squares[...] = jnp.sum(sums[...], axis=0, keepdims=True)

    def exchange(value_ref, slots, targets, sem):
        for i, target in enumerate(targets):
            remote(value_ref, slots.at[i], small_send.at[sem], small_sem.at[sem], target).start()

    def spread(value_ref, slots, places, sem):
        @pl.when(c == 1)
        def _send():
            for i, place in enumerate(places):
                for core in range(2):
                    remote(
                        value_ref, slots.at[i], small_send.at[sem], small_sem.at[sem],
                        {**place, C: core},
                    ).start()

        landed(slots, small_sem.at[sem])

    def spread_done(slots, sem):
        @pl.when(c == 1)
        def _left():
            landed(slots, small_send.at[sem])
            landed(slots, small_send.at[sem])

    hops = (0, 1, 2, 1)

    def far_first(at_x):
        places = [(kx, ky, kz) for kx in at_x for ky in range(4) for kz in range(4)]
        places = [place for place in places if any(place)]
        places.sort(key=lambda place: -sum(hops[k] for k in place))
        return [{X: step(x, kx), Y: step(y, ky), Z: step(z, kz)} for kx, ky, kz in places]

    everyone = [
        {**place, C: step2} for place in far_first(range(4)) for step2 in (c, other)
    ] + [{C: other}]
    exchange(squares, norm_p, everyone, 1)
    landed(norm_p, small_sem.at[1])
    square_sum = jnp.sum(squares[...] + jnp.sum(norm_p[...], axis=0), keepdims=True)
    clip_scale = clip_limit / jnp.maximum(jnp.sqrt(square_sum), clip_limit)

    tile = 32
    first_top = jnp.zeros((8, width), jnp.float32)
    second_top = jnp.zeros((8, width), jnp.float32)

    def moment(t, tops):
        here = pl.ds(pl.multiple_of(t * tile, tile), tile)
        clipped = clip_scale * grad[here, :]
        first = first_new[here, :] + (1.0 - beta_first) * clipped
        second = second_new[here, :] + (1.0 - beta_second) * clipped * clipped
        first_new[here, :] = first
        second_new[here, :] = second
        outs = []
        for i, (value, top) in enumerate(((jnp.abs(first), tops[0]), (second, tops[1]))):
            outs.append(jnp.maximum(top, jnp.max(value.reshape(tile // 8, 8, width), axis=0)))
            most = value[:, :128]
            for j in range(1, width // 128):
                most = jnp.maximum(most, value[:, j * 128 : (j + 1) * 128])
            rowmax[i, here, :] = most
        return tuple(outs)

    first_top, second_top = lax.fori_loop(0, grad.shape[0] // tile, moment, (first_top, second_top))
    colmax[0:1, :] = jnp.max(first_top, axis=0, keepdims=True)
    colmax[1:2, :] = jnp.max(second_top, axis=0, keepdims=True)

    exchange(colmax, col_c, [{C: other}], 2)
    first_row = jnp.max(jnp.transpose(rowmax[0]), axis=0, keepdims=True)
    first_rowmax[...] = jnp.maximum(first_row, scale_floor)
    second_rowmax[...] = jnp.max(jnp.transpose(rowmax[1]), axis=0, keepdims=True)

    landed(col_c, small_sem.at[2])
    landed(col_c, small_send.at[2])
    colmax[...] = jnp.maximum(colmax[...], col_c[0])
    spread(colmax, col_z, far_first((0,)), 3)
    result = jnp.maximum(colmax[...], jnp.max(col_z[...], axis=0))
    first_colmax[...] = jnp.maximum(result[0:1], scale_floor)
    second_colmax[...] = result[1:2]
    landed(norm_p, small_send.at[1])
    spread_done(col_z, 3)

    landed(got, got_send)
    for kind, (ref, ref_t) in enumerate((
        (sent_l, sent_lt), (sent_m, sent_mt), (sent_l2, sent_l2t), (sent_m2, sent_m2t),
    )):
        landed(ref, sends.at[kind])
        landed(ref_t, sends.at[kind + 4])


def scale(
    first_new, second_new, first_rowmax, first_colmax, second_rowmax, second_colmax,
    direction, first_scaled, second_scaled,
    first_row_out, first_col_out, second_row_out, second_col_out,
    out, out_sem, max_sem,
):
    copies = [
        pltpu.make_async_copy(ref, to, max_sem.at[i]) for i, (ref, to) in enumerate((
            (first_rowmax, first_row_out), (first_colmax, first_col_out),
            (second_rowmax, second_row_out), (second_colmax, second_col_out),
        ))
    ]
    for copy in copies:
        copy.start()
    rows, width = first_new.shape
    tile = rows // TILES
    by_row = [
        jnp.transpose(jnp.broadcast_to(ref[...], (128, rows)))
        for ref in (first_rowmax, second_rowmax)
    ]
    for t in range(TILES):
        here = slice(t * tile, (t + 1) * tile)
        for j in range(width // 128):
            cols = slice(j * 128, j * 128 + 128)
            first, second = first_new[here, cols], second_new[here, cols]
            out[0, here, cols] = first / (jnp.sqrt(second) + epsilon)
            out[1, here, cols] = first / jnp.minimum(by_row[0][here], first_colmax[:, cols])
            out[2, here, cols] = second / jnp.minimum(by_row[1][here], second_colmax[:, cols])
        for i, to in enumerate((direction, first_scaled, second_scaled)):
            copy = pltpu.make_async_copy(out.at[i, here], to.at[here], out_sem.at[t, i])
            copy.start()
            copies.append(copy)
    for copy in copies:
        copy.wait()


def local(
    grad_parts, first_codes, first_rows, first_columns, second_codes, second_rows, second_columns
):
    layer_count, _, row_count, col_count = grad_parts.shape
    entries = layer_count * lax.axis_size(X) * row_count * col_count
    clip_limit = clip_rms * math.sqrt(entries)
    own_rows = first_codes.shape[1]
    rows = own_rows * ACROSS // SLICES
    span = col_count // ACROSS
    q = span // 4
    f32, bf16 = jnp.float32, jnp.bfloat16
    shape = jax.ShapeDtypeStruct
    vmem = pltpu.VMEM
    dma = pltpu.SemaphoreType.DMA
    grads = grad_parts.reshape(2, 2, 2, 2, 2, own_rows, col_count)
    hbm_spec = pl.BlockSpec(memory_space=pltpu.HBM)
    vmem_spec = pl.BlockSpec(memory_space=pltpu.VMEM)
    n = SLICES

    def coded(count):
        return vmem((n, 2, 2, count, rows, q), jnp.int16), vmem((n, 2, 2, count, q), bf16 if count > 1 else f32)

    first_new, second_new, first_rowmax, first_colmax, second_rowmax, second_colmax = pl.pallas_call(
        functools.partial(kernel, clip_limit),
        out_shape=(
            shape((own_rows, col_count), f32), shape((own_rows, col_count), f32),
            shape((1, own_rows), f32), shape((1, col_count), f32),
            shape((1, own_rows), f32), shape((1, col_count), f32),
        ),
        in_specs=[hbm_spec] * 7,
        out_specs=[vmem_spec] * 6,
        scratch_shapes=[
            vmem((n, 2, 2, 2, 2, rows, span), bf16),
            vmem((n, 2, 2, 2, 2, rows, span), bf16),
            *coded(8), *coded(8),
            *coded(4), *coded(4),
            vmem((n, 2, 2, 4, rows, q), f32),
            *coded(2), *coded(2),
            *coded(1), *coded(1),
            vmem((2, own_rows, col_count), jnp.int32),
            vmem((own_rows, col_count), f32),
            vmem((8, 128), f32),
            vmem((1, 128), f32),
            vmem((1, 1, 128), f32),
            vmem((127, 1, 128), f32),
            vmem((2, own_rows, 128), f32),
            vmem((2, col_count), f32),
            vmem((1, 2, col_count), f32),
            vmem((15, 2, col_count), f32),
            *[vmem((1, own_rows), f32), vmem((1, col_count), f32)] * 2,
            vmem((1, 16 * (rows + 1) * q), f32),
            vmem((2, 2, 2, 2, rows, span), bf16),
            dma((3,)), dma((n + 1,)), dma((2,)),
            dma((n,)), dma((n,)), dma((n,)), dma((n,)), dma((4,)),
            dma, dma((8,)), dma((4,)), pltpu.SemaphoreType.REGULAR((ROUNDS,)),
        ],
        compiler_params=pltpu.CompilerParams(
            collective_id=0, has_side_effects=True, vmem_limit_bytes=46 * 2**20
        ),
        name="clipped_adam",
    )(
        *(
            pltpu.with_memory_space_constraint(v, pltpu.HBM)
            for v in (
                grads, first_codes[0], first_rows, first_columns, second_codes[0], second_rows,
                second_columns,
            )
        )
    )
    big, by_row, by_col = (shape(s, f32) for s in ((own_rows, col_count), (1, own_rows), (1, col_count)))
    direction, first_scaled, second_scaled, *maxima = pl.pallas_call(
        scale,
        out_shape=(big, big, big, by_row, by_col, by_row, by_col),
        in_specs=[vmem_spec] * 6,
        out_specs=[hbm_spec] * 7,
        scratch_shapes=[vmem((3, own_rows, col_count), f32), dma((TILES, 3)), dma((4,))],
        compiler_params=pltpu.CompilerParams(vmem_limit_bytes=12 * 2**20),
        name="scale",
    )(first_new, second_new, first_rowmax, first_colmax, second_rowmax, second_colmax)
    return direction[None], first_scaled[None], second_scaled[None], *maxima


def solution(mesh):
    torus = Mesh(mesh.devices.reshape(mesh.shape["section"], 4, 4, 2), (X, Y, Z, C))
    placed = (
        P(X, FSDP, None, None),
        P(X, FSDP, None),
        P(X, FSDP),
        P(X, None),
        P(X, FSDP, None),
        P(X, FSDP),
        P(X, None),
    )
    return jax.shard_map(
        local,
        mesh=torus,
        in_specs=placed,
        out_specs=(
            P(X, FSDP, None), P(X, FSDP, None), P(X, FSDP, None),
            P(X, FSDP), P(X, None), P(X, FSDP), P(X, None),
        ),
        check_vma=False,
    )
```

```python
import functools
import math

import jax
import jax.numpy as jnp
from jax import lax
from jax.experimental import pallas as pl
from jax.experimental.pallas import tpu as pltpu
from jax.sharding import Mesh
from jax.sharding import PartitionSpec as P

Y, Z, C, X = "fsdp_0", "fsdp_1", "fsdp_2", "section"
FSDP = (Y, Z, C)
MESH = pl.DeviceIdType.MESH

beta_first = 0.9
beta_second = 0.999
clip_rms = 3.0
epsilon = 1e-08
scale_floor = 0.001

SLICES = 8
ACROSS = 2
AHEAD = 3
ROUNDS = 6
TILES = 4
LEVELS = 32766.0
TINY = 2e-34
DIRS = ((0, 1), (1, 3))


def remote(src, dst, send, recv, device):
    return pltpu.make_async_remote_copy(
        src_ref=src, dst_ref=dst, send_sem=send, recv_sem=recv,
        device_id=device, device_id_type=MESH,
    )


def landed(buf, sem):
    pltpu.make_async_copy(buf, buf, sem).wait()


def put(values, codes, tops, key):
    rows = []
    for i, value in enumerate(values):
        top = jnp.maximum(jnp.max(jnp.abs(value), axis=0, keepdims=True), TINY) * 1.008
        top = top.astype(jnp.bfloat16).astype(jnp.float32)
        scaled = jnp.round(value * (LEVELS / top))
        codes[(*key, i)] = scaled.astype(jnp.int32).astype(jnp.int16)
        rows.append(top)
    tops[key] = jnp.concatenate(rows, axis=0).astype(tops.dtype)


def take(codes, tops, key, i):
    unit = tops[key].astype(jnp.float32)[i : i + 1] * (1.0 / LEVELS)
    return codes[(*key, i)].astype(jnp.int32).astype(jnp.float32) * unit


def kernel(
    clip_limit,
    grads, first_codes, first_rows, first_columns, second_codes, second_rows, second_columns,
    direction, first_new, second_new, first_rowmax, first_colmax, second_rowmax, second_colmax,
    own, got, sent_l, sent_lt, came_l, came_lt, sent_m, sent_mt, came_m, came_mt, total,
    sent_l2, sent_l2t, came_l2, came_l2t, sent_m2, sent_m2t, came_m2, came_m2t,
    codes, grad, sums, squares, norm_c, norm_p, rowmax, colmax, col_c, col_z,
    first_r, first_c, second_r, second_c, words_ref, gift,
    own_sem, got_sem, code_sem, l_sem, m_sem, l2_sem, m2_sem, small_sem,
    got_send, sends, small_send, word_sem,
):
    slices, *_, rows, span = own.shape
    width = grad.shape[1]
    across = width // span
    quarter = span // 4
    y, z, c, x = (lax.axis_index(a) for a in (Y, Z, C, X))
    at = (y, z)
    names = (Y, Z)
    other = 1 - c

    def step(v, k):
        return lax.rem(v + k, 4)

    barrier = pltpu.get_barrier_semaphore()
    peers = [{C: other}]
    for axis, name in enumerate(names):
        for k in (1, 3):
            peers.append({name: step(at[axis], k), C: other})
    for k in (1, 3):
        peers.append({X: step(x, k)})
    for peer in peers:
        pl.semaphore_signal(barrier, inc=1, device_id=peer, device_id_type=MESH)

    def block(p):
        down = pl.ds(pl.multiple_of(p // across * rows, rows), rows)
        return down, pl.ds(pl.multiple_of(p % across * span, span), span)

    def pieces(p, core):
        for i in range(2):
            for j in range(2):
                whose = lax.rem(core + y + z + i + j, 2)
                yield grads.at[:, i, :, j, whose, *block(p)], (slice(None), i, slice(None), j)

    for piece, where in pieces(0, other):
        pltpu.make_async_copy(piece, gift.at[where], own_sem.at[2]).start()

    def load(p, sem):
        for piece, where in pieces(p, c):
            pltpu.make_async_copy(piece, own.at[(p, *where)], own_sem.at[sem]).start()
        return sem

    load(0, 0)
    lax.fori_loop(1, slices, load, 1)
    small = (
        (first_rows, first_r), (first_columns, first_c), (second_rows, second_r),
        (second_columns, second_c),
    )
    for i, (ref, to) in enumerate((
        (first_codes, codes.at[0]), (second_codes, codes.at[1]), *small,
    )):
        pltpu.make_async_copy(ref, to, code_sem.at[0 if i < 2 else 1]).start()

    pl.semaphore_wait(barrier, len(peers))
    def spread_word(p):
        @pl.when((p > 0) & (p <= ROUNDS))
        def _hear():
            pl.semaphore_wait(word_sem.at[p - 1], len(peers))

        @pl.when(p < ROUNDS)
        def _tell():
            for peer in peers:
                pl.semaphore_signal(
                    word_sem.at[p], inc=1, device_id=peer, device_id_type=MESH
                )

    def give(p, _):
        for piece, where in pieces(p, other):
            remote(piece, got.at[(p, *where)], got_send, got_sem.at[p], {C: other}).start()
        return _

    def columns(axis, slot):
        return pl.ds((2 * axis + slot) * quarter, quarter)

    def block_of(axis, index, slot):
        where = (index // 2, index % 2)
        around = (slice(None), slice(None))
        where = (*where, *around) if axis == 0 else (*around, *where)
        return (*where, slice(None), columns(axis, slot))

    def gift_block(axis, index, slot, sem):
        where = block_of(axis, index, slot)
        remote(
            gift.at[where], got.at[(0, *where)], got_send, got_sem.at[sem], {C: other}
        ).start()

    landed(gift, own_sem.at[2])
    for axis in (0, 1):
        for slot, k in DIRS:
            gift_block(axis, step(at[axis], 2), slot, slices + 2 * axis + slot)
            gift_block(axis, step(at[axis], k), 1 - slot, slices + 2 * axis + slot)
    for axis in (0, 1):
        for slot, k in DIRS:
            gift_block(axis, step(at[axis], k), slot, 0)
            gift_block(axis, at[axis], slot, 0)
    lax.fori_loop(1, AHEAD + 1, give, 0)

    def blocks_landed(count, sem):
        landed(words_ref.at[:, pl.ds(0, count * 4 * rows * quarter // 2)], sem)

    def pair(p, axis, index, j, slot):
        index, j = (index // 2, index % 2), (j // 2, j % 2)
        where = (*index, *j) if axis == 0 else (*j, *index)
        where = (p, *where, slice(None), columns(axis, slot))
        return own[where].astype(jnp.float32) + got[where].astype(jnp.float32)

    def send(kind, key, ref, ref_t, out, out_t, sem, device):
        remote(ref.at[key], out.at[key], sends.at[kind], sem, device).start()
        remote(ref_t.at[key], out_t.at[key], sends.at[kind + 4], sem, device).start()

    def arrived(messages, slabs, sem):
        words = messages * (slabs * rows * quarter // 2 + max(slabs, 2) * quarter // 2)
        landed(words_ref.at[:, pl.ds(0, words)], sem)

    def leaves(p, ready):
        @pl.when(p + AHEAD + 1 < slices)
        def _next():
            give(p + AHEAD + 1, 0)

        for axis in (0, 1):
            me = at[axis]
            for slot, k in DIRS:
                ready(axis, slot)
                values = [pair(p, axis, step(me, 2), j, slot) for j in range(4)]
                values += [pair(p, axis, step(me, k), j, 1 - slot) for j in range(4)]
                put(values, sent_l, sent_lt, (p, axis, slot))
                send(0, (p, axis, slot), sent_l, sent_lt, came_l, came_lt, l_sem.at[p],
                     {names[axis]: step(me, k), C: other})

    def first_ready(axis, slot):
        if axis == 0 and slot == 0:
            landed(own.at[0], own_sem.at[0])
        blocks_landed(2, got_sem.at[slices + 2 * axis + slot])

    def later_ready(p, axis, slot):
        if axis == 0 and slot == 0:
            landed(got.at[p], got_sem.at[p])

    def later(p, _):
        leaves(p, functools.partial(later_ready, p))
        return _

    leaves(0, first_ready)
    landed(own.at[pl.ds(1, slices - 1)], own_sem.at[1])
    blocks_landed(8, got_sem.at[0])
    lax.fori_loop(1, AHEAD, later, 0)

    def middles(p, _):
        arrived(4, 8, l_sem.at[p])
        for axis in (0, 1):
            me = at[axis]
            for slot, k in DIRS:
                key = (p, axis, slot)
                values = [
                    pair(p, axis, step(me, k), j, slot) + take(came_l, came_lt, key, j)
                    for j in range(4)
                ]
                put(values, sent_m, sent_mt, key)
                send(1, key, sent_m, sent_mt, came_m, came_mt, m_sem.at[p],
                     {names[axis]: step(me, k), C: other})
        return _

    def both(p, _):
        spread_word(p)

        @pl.when(p + AHEAD < slices)
        def _next():
            later(p + AHEAD, 0)

        return middles(p, _)

    lax.fori_loop(0, slices, both, 0)

    landed(codes, code_sem.at[0])
    landed(words_ref.at[:, pl.ds(0, 2 * (grad.shape[0] + width))], code_sem.at[1])
    for i, (row_ref, col_ref, out, factor) in enumerate((
        (first_r, first_c, first_new, beta_first / 7.0),
        (second_r, second_c, second_new, beta_second / 15.0),
    )):
        row_count = row_ref.shape[1]
        by_row = jnp.transpose(jnp.broadcast_to(row_ref[...], (128, row_count)))
        for j in range(width // 128):
            cols = pl.ds(j * 128, 128)
            bound = jnp.minimum(by_row, col_ref[:, cols])
            out[:, cols] = codes[i, :, cols].astype(jnp.float32) * factor * bound

    def totals(p, _):
        arrived(4, 4, m_sem.at[p])
        for axis in (0, 1):
            me, over, way = at[axis], at[1 - axis], names[1 - axis]
            for slot, k in DIRS:
                for j in range(4):
                    total[p, axis, slot, j] = (
                        pair(p, axis, me, j, slot)
                        + take(came_m, came_mt, (p, axis, slot), j)
                        + take(came_l, came_lt, (p, axis, 1 - slot), 4 + j)
                    )
            for slot, k in DIRS:
                values = [
                    total[p, axis, which, step(over, index)]
                    for which, index in ((slot, 2), (1 - slot, k))
                ]
                put(values, sent_l2, sent_l2t, (p, axis, slot))
                send(2, (p, axis, slot), sent_l2, sent_l2t, came_l2, came_l2t, l2_sem.at[p],
                     {way: step(over, k), C: other})
        return _

    lax.fori_loop(0, slices, totals, 0)

    def middles2(p, _):
        arrived(4, 2, l2_sem.at[p])
        for axis in (0, 1):
            over, way = at[1 - axis], names[1 - axis]
            for slot, k in DIRS:
                key = (p, axis, slot)
                value = total[p, axis, slot, step(over, k)] + take(came_l2, came_l2t, key, 0)
                put([value], sent_m2, sent_m2t, key)
                send(3, key, sent_m2, sent_m2t, came_m2, came_m2t, m2_sem.at[p],
                     {way: step(over, k), C: other})
        return _

    lax.fori_loop(0, slices, middles2, 0)

    sums[...] = jnp.zeros_like(sums)

    def finish(p, _):
        arrived(4, 1, m2_sem.at[p])
        for axis in (0, 1):
            over = at[1 - axis]
            for slot, k in DIRS:
                value = (
                    total[p, axis, slot, over]
                    + take(came_m2, came_m2t, (p, axis, slot), 0)
                    + take(came_l2, came_l2t, (p, axis, 1 - slot), 1)
                )
                here = pl.multiple_of(p % across * span + (2 * axis + slot) * quarter, quarter)
                grad[block(p)[0], pl.ds(here, quarter)] = value
                sq = value * value
                part = sq[:, :128]
                for j in range(1, quarter // 128):
                    part = part + sq[:, j * 128 : (j + 1) * 128]
                sums[...] += jnp.sum(part.reshape(rows // 8, 8, 128), axis=0)
        return _

    lax.fori_loop(0, slices, finish, 0)
    squares[...] = jnp.sum(sums[...], axis=0, keepdims=True)

    def exchange(value_ref, slots, targets, sem):
        for i, target in enumerate(targets):
            remote(value_ref, slots.at[i], small_send.at[sem], small_sem.at[sem], target).start()

    def send_spread(value_ref, slots, places, sem):
        @pl.when(c == 1)
        def _send():
            for i, place in enumerate(places):
                for core in range(2):
                    remote(
                        value_ref, slots.at[i], small_send.at[sem], small_sem.at[sem],
                        {**place, C: core},
                    ).start()

    def spread_done(slots, sem):
        @pl.when(c == 1)
        def _left():
            landed(slots, small_send.at[sem])
            landed(slots, small_send.at[sem])

    hops = (0, 1, 2, 1)

    def far_first(at_x):
        places = [(kx, ky, kz) for kx in at_x for ky in range(4) for kz in range(4)]
        places = [place for place in places if any(place)]
        places.sort(key=lambda place: -sum(hops[k] for k in place))
        return [{X: step(x, kx), Y: step(y, ky), Z: step(z, kz)} for kx, ky, kz in places]

    everyone = [
        {**place, C: step2} for place in far_first(range(4)) for step2 in (c, other)
    ] + [{C: other}]
    exchange(squares, norm_p, everyone, 1)
    landed(norm_p, small_sem.at[1])
    square_sum = jnp.sum(squares[...] + jnp.sum(norm_p[...], axis=0), keepdims=True)
    clip_scale = clip_limit / jnp.maximum(jnp.sqrt(square_sum), clip_limit)

    tile = 32
    first_top = jnp.zeros((8, width), jnp.float32)
    second_top = jnp.zeros((8, width), jnp.float32)

    def moment(t, tops):
        here = pl.ds(pl.multiple_of(t * tile, tile), tile)
        clipped = clip_scale * grad[here, :]
        first = first_new[here, :] + (1.0 - beta_first) * clipped
        second = second_new[here, :] + (1.0 - beta_second) * clipped * clipped
        first_new[here, :] = first
        second_new[here, :] = second
        outs = []
        for i, (value, top) in enumerate(((jnp.abs(first), tops[0]), (second, tops[1]))):
            outs.append(jnp.maximum(top, jnp.max(value.reshape(tile // 8, 8, width), axis=0)))
            most = value[:, :128]
            for j in range(1, width // 128):
                most = jnp.maximum(most, value[:, j * 128 : (j + 1) * 128])
            rowmax[i, here, :] = most
        return tuple(outs)

    first_top, second_top = lax.fori_loop(0, grad.shape[0] // tile, moment, (first_top, second_top))
    colmax[0:1, :] = jnp.max(first_top, axis=0, keepdims=True)
    colmax[1:2, :] = jnp.max(second_top, axis=0, keepdims=True)

    exchange(colmax, col_c, [{C: other}], 2)
    first_row = jnp.max(jnp.transpose(rowmax[0]), axis=0, keepdims=True)
    first_rowmax[...] = jnp.maximum(first_row, scale_floor)
    second_rowmax[...] = jnp.max(jnp.transpose(rowmax[1]), axis=0, keepdims=True)

    landed(col_c, small_sem.at[2])
    landed(col_c, small_send.at[2])
    colmax[...] = jnp.maximum(colmax[...], col_c[0])
    send_spread(colmax, col_z, far_first((0,)), 3)

    def direct(t, _):
        here = pl.ds(pl.multiple_of(t * tile, tile), tile)
        direction[here, :] = first_new[here, :] / (jnp.sqrt(second_new[here, :]) + epsilon)
        return _

    lax.fori_loop(0, grad.shape[0] // tile, direct, 0)
    landed(col_z, small_sem.at[3])
    result = jnp.maximum(colmax[...], jnp.max(col_z[...], axis=0))
    first_colmax[...] = jnp.maximum(result[0:1], scale_floor)
    second_colmax[...] = result[1:2]
    landed(norm_p, small_send.at[1])
    spread_done(col_z, 3)

    landed(got, got_send)
    for kind, (ref, ref_t) in enumerate((
        (sent_l, sent_lt), (sent_m, sent_mt), (sent_l2, sent_l2t), (sent_m2, sent_m2t),
    )):
        landed(ref, sends.at[kind])
        landed(ref_t, sends.at[kind + 4])


def scale(
    direction, first_new, second_new, first_rowmax, first_colmax, second_rowmax, second_colmax,
    direction_out, first_scaled, second_scaled,
    first_row_out, first_col_out, second_row_out, second_col_out,
    out, out_sem, max_sem,
):
    copies = [
        pltpu.make_async_copy(ref, to, max_sem.at[i]) for i, (ref, to) in enumerate((
            (direction, direction_out),
            (first_rowmax, first_row_out), (first_colmax, first_col_out),
            (second_rowmax, second_row_out), (second_colmax, second_col_out),
        ))
    ]
    for copy in copies:
        copy.start()
    rows, width = first_new.shape
    tile = rows // TILES
    for i, (value, row, col, to) in enumerate((
        (first_new, first_rowmax, first_colmax, first_scaled),
        (second_new, second_rowmax, second_colmax, second_scaled),
    )):
        by_row = jnp.transpose(jnp.broadcast_to(1.0 / row[...], (128, rows)))
        by_col = 1.0 / col[...]
        for t in range(TILES):
            here = slice(t * tile, (t + 1) * tile)
            for j in range(width // 128):
                cols = slice(j * 128, j * 128 + 128)
                out[i, here, cols] = value[here, cols] * jnp.maximum(by_row[here], by_col[:, cols])
            copy = pltpu.make_async_copy(out.at[i, here], to.at[here], out_sem.at[t, i])
            copy.start()
            copies.append(copy)
    for copy in copies:
        copy.wait()


def local(
    grad_parts, first_codes, first_rows, first_columns, second_codes, second_rows, second_columns
):
    layer_count, _, row_count, col_count = grad_parts.shape
    entries = layer_count * lax.axis_size(X) * row_count * col_count
    clip_limit = clip_rms * math.sqrt(entries)
    own_rows = first_codes.shape[1]
    rows = own_rows * ACROSS // SLICES
    span = col_count // ACROSS
    q = span // 4
    f32, bf16 = jnp.float32, jnp.bfloat16
    shape = jax.ShapeDtypeStruct
    vmem = pltpu.VMEM
    dma = pltpu.SemaphoreType.DMA
    grads = grad_parts.reshape(2, 2, 2, 2, 2, own_rows, col_count)
    hbm_spec = pl.BlockSpec(memory_space=pltpu.HBM)
    vmem_spec = pl.BlockSpec(memory_space=pltpu.VMEM)
    n = SLICES

    def coded(count):
        return vmem((n, 2, 2, count, rows, q), jnp.int16), vmem((n, 2, 2, count, q), bf16 if count > 1 else f32)

    results = pl.pallas_call(
        functools.partial(kernel, clip_limit),
        out_shape=(
            *[shape((own_rows, col_count), f32)] * 3,
            shape((1, own_rows), f32), shape((1, col_count), f32),
            shape((1, own_rows), f32), shape((1, col_count), f32),
        ),
        in_specs=[hbm_spec] * 7,
        out_specs=[vmem_spec] * 7,
        scratch_shapes=[
            vmem((n, 2, 2, 2, 2, rows, span), bf16),
            vmem((n, 2, 2, 2, 2, rows, span), bf16),
            *coded(8), *coded(8),
            *coded(4), *coded(4),
            vmem((n, 2, 2, 4, rows, q), f32),
            *coded(2), *coded(2),
            *coded(1), *coded(1),
            vmem((2, own_rows, col_count), jnp.int32),
            vmem((own_rows, col_count), f32),
            vmem((8, 128), f32),
            vmem((1, 128), f32),
            vmem((1, 1, 128), f32),
            vmem((127, 1, 128), f32),
            vmem((2, own_rows, 128), f32),
            vmem((2, col_count), f32),
            vmem((1, 2, col_count), f32),
            vmem((15, 2, col_count), f32),
            *[vmem((1, own_rows), f32), vmem((1, col_count), f32)] * 2,
            vmem((1, 16 * (rows + 1) * q), f32),
            vmem((2, 2, 2, 2, rows, span), bf16),
            dma((3,)), dma((n + 4,)), dma((2,)),
            dma((n,)), dma((n,)), dma((n,)), dma((n,)), dma((4,)),
            dma, dma((8,)), dma((4,)), pltpu.SemaphoreType.REGULAR((ROUNDS,)),
        ],
        compiler_params=pltpu.CompilerParams(
            collective_id=0, has_side_effects=True, vmem_limit_bytes=46 * 2**20
        ),
        name="clipped_adam",
    )(
        *(
            pltpu.with_memory_space_constraint(v, pltpu.HBM)
            for v in (
                grads, first_codes[0], first_rows, first_columns, second_codes[0], second_rows,
                second_columns,
            )
        )
    )
    big, by_row, by_col = (shape(s, f32) for s in ((own_rows, col_count), (1, own_rows), (1, col_count)))
    direction, first_scaled, second_scaled, *maxima = pl.pallas_call(
        scale,
        out_shape=(big, big, big, by_row, by_col, by_row, by_col),
        in_specs=[vmem_spec] * 7,
        out_specs=[hbm_spec] * 7,
        scratch_shapes=[vmem((2, own_rows, col_count), f32), dma((TILES, 2)), dma((5,))],
        compiler_params=pltpu.CompilerParams(vmem_limit_bytes=12 * 2**20),
        name="scale",
    )(*results)
    return direction[None], first_scaled[None], second_scaled[None], *maxima


def solution(mesh):
    torus = Mesh(mesh.devices.reshape(mesh.shape["section"], 4, 4, 2), (X, Y, Z, C))
    placed = (
        P(X, FSDP, None, None),
        P(X, FSDP, None),
        P(X, FSDP),
        P(X, None),
        P(X, FSDP, None),
        P(X, FSDP),
        P(X, None),
    )
    return jax.shard_map(
        local,
        mesh=torus,
        in_specs=placed,
        out_specs=(
            P(X, FSDP, None), P(X, FSDP, None), P(X, FSDP, None),
            P(X, FSDP), P(X, None), P(X, FSDP), P(X, None),
        ),
        check_vma=False,
    )
```

```python
import functools
import math

import jax
import jax.numpy as jnp
from jax import lax
from jax.experimental import pallas as pl
from jax.experimental.pallas import tpu as pltpu
from jax.sharding import Mesh
from jax.sharding import PartitionSpec as P

Y, Z, C, X = "fsdp_0", "fsdp_1", "fsdp_2", "section"
FSDP = (Y, Z, C)
MESH = pl.DeviceIdType.MESH

beta_first = 0.9
beta_second = 0.999
clip_rms = 3.0
epsilon = 1e-08
scale_floor = 0.001

SLICES = 8
ACROSS = 2
AHEAD = 3
ROUNDS = 6
TILES = 4
LEVELS = 32766.0
TINY = 2e-34
DIRS = ((0, 1), (1, 3))


def remote(src, dst, send, recv, device):
    return pltpu.make_async_remote_copy(
        src_ref=src, dst_ref=dst, send_sem=send, recv_sem=recv,
        device_id=device, device_id_type=MESH,
    )


def landed(buf, sem):
    pltpu.make_async_copy(buf, buf, sem).wait()


def put(values, codes, tops, key):
    rows = []
    for i, value in enumerate(values):
        top = jnp.maximum(jnp.max(jnp.abs(value), axis=0, keepdims=True), TINY) * 1.008
        top = top.astype(jnp.bfloat16).astype(jnp.float32)
        scaled = jnp.round(value * (LEVELS / top))
        codes[(*key, i)] = scaled.astype(jnp.int32).astype(jnp.int16)
        rows.append(top)
    tops[key] = jnp.concatenate(rows, axis=0).astype(tops.dtype)


def take(codes, tops, key, i):
    unit = tops[key].astype(jnp.float32)[i : i + 1] * (1.0 / LEVELS)
    return codes[(*key, i)].astype(jnp.int32).astype(jnp.float32) * unit


def kernel(
    clip_limit,
    grads, first_codes, first_rows, first_columns, second_codes, second_rows, second_columns,
    direction, first_new, second_new, first_rowmax, first_colmax, second_rowmax, second_colmax,
    own, got, sent_l, sent_lt, came_l, came_lt, sent_m, sent_mt, came_m, came_mt, total,
    sent_l2, sent_l2t, came_l2, came_l2t, sent_m2, sent_m2t, came_m2, came_m2t,
    codes, grad, sums, squares, norm_c, norm_p, rowmax, colmax, col_c, col_z,
    first_r, first_c, second_r, second_c, words_ref, gift,
    own_sem, got_sem, code_sem, l_sem, m_sem, l2_sem, m2_sem, small_sem,
    got_send, sends, small_send, word_sem,
):
    slices, *_, rows, span = own.shape
    width = grad.shape[1]
    across = width // span
    quarter = span // 4
    y, z, c, x = (lax.axis_index(a) for a in (Y, Z, C, X))
    at = (y, z)
    names = (Y, Z)
    other = 1 - c

    def step(v, k):
        return lax.rem(v + k, 4)

    barrier = pltpu.get_barrier_semaphore()
    peers = [{C: other}]
    for axis, name in enumerate(names):
        for k in (1, 3):
            peers.append({name: step(at[axis], k), C: other})
    for k in (1, 3):
        peers.append({X: step(x, k)})
    for peer in peers:
        pl.semaphore_signal(barrier, inc=1, device_id=peer, device_id_type=MESH)

    def block(p):
        down = pl.ds(pl.multiple_of(p // across * rows, rows), rows)
        return down, pl.ds(pl.multiple_of(p % across * span, span), span)

    def pieces(p, core):
        for i in range(2):
            for j in range(2):
                whose = lax.rem(core + y + z + i + j, 2)
                yield grads.at[:, i, :, j, whose, *block(p)], (slice(None), i, slice(None), j)

    for piece, where in pieces(0, other):
        pltpu.make_async_copy(piece, gift.at[where], own_sem.at[2]).start()

    def load(p, sem):
        for piece, where in pieces(p, c):
            pltpu.make_async_copy(piece, own.at[(p, *where)], own_sem.at[sem]).start()
        return sem

    load(0, 0)
    lax.fori_loop(1, slices, load, 1)
    small = (
        (first_rows, first_r), (first_columns, first_c), (second_rows, second_r),
        (second_columns, second_c),
    )
    for i, (ref, to) in enumerate((
        (first_codes, codes.at[0]), (second_codes, codes.at[1]), *small,
    )):
        pltpu.make_async_copy(ref, to, code_sem.at[0 if i < 2 else 1]).start()

    pl.semaphore_wait(barrier, len(peers))
    def spread_word(p):
        @pl.when((p > 0) & (p <= ROUNDS))
        def _hear():
            pl.semaphore_wait(word_sem.at[p - 1], len(peers))

        @pl.when(p < ROUNDS)
        def _tell():
            for peer in peers:
                pl.semaphore_signal(
                    word_sem.at[p], inc=1, device_id=peer, device_id_type=MESH
                )

    def give(p, _):
        for piece, where in pieces(p, other):
            remote(piece, got.at[(p, *where)], got_send, got_sem.at[p], {C: other}).start()
        return _

    def columns(axis, slot):
        return pl.ds((2 * axis + slot) * quarter, quarter)

    def block_of(axis, index, slot):
        where = (index // 2, index % 2)
        around = (slice(None), slice(None))
        where = (*where, *around) if axis == 0 else (*around, *where)
        return (*where, slice(None), columns(axis, slot))

    def gift_block(axis, index, slot, sem):
        where = block_of(axis, index, slot)
        remote(
            gift.at[where], got.at[(0, *where)], got_send, got_sem.at[sem], {C: other}
        ).start()

    landed(gift, own_sem.at[2])
    for axis in (0, 1):
        for slot, k in DIRS:
            gift_block(axis, step(at[axis], 2), slot, slices + 2 * axis + slot)
            gift_block(axis, step(at[axis], k), 1 - slot, slices + 2 * axis + slot)
    for axis in (0, 1):
        for slot, k in DIRS:
            gift_block(axis, step(at[axis], k), slot, 0)
            gift_block(axis, at[axis], slot, 0)
    lax.fori_loop(1, AHEAD + 1, give, 0)

    def blocks_landed(count, sem):
        landed(words_ref.at[:, pl.ds(0, count * 4 * rows * quarter // 2)], sem)

    def pair(p, axis, index, j, slot):
        index, j = (index // 2, index % 2), (j // 2, j % 2)
        where = (*index, *j) if axis == 0 else (*j, *index)
        where = (p, *where, slice(None), columns(axis, slot))
        return own[where].astype(jnp.float32) + got[where].astype(jnp.float32)

    def send(kind, key, ref, ref_t, out, out_t, sem, device):
        remote(ref.at[key], out.at[key], sends.at[kind], sem, device).start()
        remote(ref_t.at[key], out_t.at[key], sends.at[kind + 4], sem, device).start()

    def arrived(messages, slabs, sem):
        words = messages * (slabs * rows * quarter // 2 + max(slabs, 2) * quarter // 2)
        landed(words_ref.at[:, pl.ds(0, words)], sem)

    def leaves(p, ready):
        @pl.when(p + AHEAD + 1 < slices)
        def _next():
            give(p + AHEAD + 1, 0)

        for axis in (0, 1):
            me = at[axis]
            for slot, k in DIRS:
                ready(axis, slot)
                values = [pair(p, axis, step(me, 2), j, slot) for j in range(4)]
                values += [pair(p, axis, step(me, k), j, 1 - slot) for j in range(4)]
                put(values, sent_l, sent_lt, (p, axis, slot))
                send(0, (p, axis, slot), sent_l, sent_lt, came_l, came_lt, l_sem.at[p],
                     {names[axis]: step(me, k), C: other})

    def first_ready(axis, slot):
        if axis == 0 and slot == 0:
            landed(own.at[0], own_sem.at[0])
        blocks_landed(2, got_sem.at[slices + 2 * axis + slot])

    def later_ready(p, axis, slot):
        if axis == 0 and slot == 0:
            landed(got.at[p], got_sem.at[p])

    def later(p, _):
        leaves(p, functools.partial(later_ready, p))
        return _

    leaves(0, first_ready)
    landed(own.at[pl.ds(1, slices - 1)], own_sem.at[1])
    blocks_landed(8, got_sem.at[0])
    lax.fori_loop(1, AHEAD, later, 0)

    def middles(p, _):
        arrived(4, 8, l_sem.at[p])
        for axis in (0, 1):
            me = at[axis]
            for slot, k in DIRS:
                key = (p, axis, slot)
                values = [
                    pair(p, axis, step(me, k), j, slot) + take(came_l, came_lt, key, j)
                    for j in range(4)
                ]
                put(values, sent_m, sent_mt, key)
                send(1, key, sent_m, sent_mt, came_m, came_mt, m_sem.at[p],
                     {names[axis]: step(me, k), C: other})
        return _

    def both(p, _):
        spread_word(p)

        @pl.when(p + AHEAD < slices)
        def _next():
            later(p + AHEAD, 0)

        return middles(p, _)

    lax.fori_loop(0, slices, both, 0)

    landed(codes, code_sem.at[0])
    landed(words_ref.at[:, pl.ds(0, 2 * (grad.shape[0] + width))], code_sem.at[1])
    for i, (row_ref, col_ref, out, factor) in enumerate((
        (first_r, first_c, first_new, beta_first / 7.0),
        (second_r, second_c, second_new, beta_second / 15.0),
    )):
        row_count = row_ref.shape[1]
        by_row = jnp.transpose(jnp.broadcast_to(row_ref[...], (128, row_count)))
        for j in range(width // 128):
            cols = pl.ds(j * 128, 128)
            bound = jnp.minimum(by_row, col_ref[:, cols])
            out[:, cols] = codes[i, :, cols].astype(jnp.float32) * factor * bound

    def totals(p, _):
        arrived(4, 4, m_sem.at[p])
        for axis in (0, 1):
            me, over, way = at[axis], at[1 - axis], names[1 - axis]
            for slot, k in DIRS:
                for j in range(4):
                    total[p, axis, slot, j] = (
                        pair(p, axis, me, j, slot)
                        + take(came_m, came_mt, (p, axis, slot), j)
                        + take(came_l, came_lt, (p, axis, 1 - slot), 4 + j)
                    )
            for slot, k in DIRS:
                values = [
                    total[p, axis, which, step(over, index)]
                    for which, index in ((slot, 2), (1 - slot, k))
                ]
                put(values, sent_l2, sent_l2t, (p, axis, slot))
                send(2, (p, axis, slot), sent_l2, sent_l2t, came_l2, came_l2t, l2_sem.at[p],
                     {way: step(over, k), C: other})
        return _

    lax.fori_loop(0, slices, totals, 0)

    def middles2(p, _):
        arrived(4, 2, l2_sem.at[p])
        for axis in (0, 1):
            over, way = at[1 - axis], names[1 - axis]
            for slot, k in DIRS:
                key = (p, axis, slot)
                value = total[p, axis, slot, step(over, k)] + take(came_l2, came_l2t, key, 0)
                put([value], sent_m2, sent_m2t, key)
                send(3, key, sent_m2, sent_m2t, came_m2, came_m2t, m2_sem.at[p],
                     {way: step(over, k), C: other})
        return _

    lax.fori_loop(0, slices, middles2, 0)

    sums[...] = jnp.zeros_like(sums)

    def finish(p, _):
        arrived(4, 1, m2_sem.at[p])
        for axis in (0, 1):
            over = at[1 - axis]
            for slot, k in DIRS:
                value = (
                    total[p, axis, slot, over]
                    + take(came_m2, came_m2t, (p, axis, slot), 0)
                    + take(came_l2, came_l2t, (p, axis, 1 - slot), 1)
                )
                here = pl.multiple_of(p % across * span + (2 * axis + slot) * quarter, quarter)
                grad[block(p)[0], pl.ds(here, quarter)] = value
                sq = value * value
                part = sq[:, :128]
                for j in range(1, quarter // 128):
                    part = part + sq[:, j * 128 : (j + 1) * 128]
                sums[...] += jnp.sum(part.reshape(rows // 8, 8, 128), axis=0)
        return _

    lax.fori_loop(0, slices, finish, 0)
    squares[...] = jnp.sum(sums[...], axis=0, keepdims=True)

    def exchange(value_ref, slots, targets, sem):
        for i, target in enumerate(targets):
            remote(value_ref, slots.at[i], small_send.at[sem], small_sem.at[sem], target).start()

    def send_spread(value_ref, slots, places, sem):
        @pl.when(c == 1)
        def _send():
            for i, place in enumerate(places):
                for core in range(2):
                    remote(
                        value_ref, slots.at[i], small_send.at[sem], small_sem.at[sem],
                        {**place, C: core},
                    ).start()

    def spread_done(slots, sem):
        @pl.when(c == 1)
        def _left():
            landed(slots, small_send.at[sem])
            landed(slots, small_send.at[sem])

    hops = (0, 1, 2, 1)

    def far_first(at_x):
        places = [(kx, ky, kz) for kx in at_x for ky in range(4) for kz in range(4)]
        places = [place for place in places if any(place)]
        places.sort(key=lambda place: -sum(hops[k] for k in place))
        return [{X: step(x, kx), Y: step(y, ky), Z: step(z, kz)} for kx, ky, kz in places]

    everyone = [
        {**place, C: step2} for place in far_first(range(4)) for step2 in (c, other)
    ] + [{C: other}]
    exchange(squares, norm_p, everyone, 1)
    landed(norm_p, small_sem.at[1])
    square_sum = jnp.sum(squares[...] + jnp.sum(norm_p[...], axis=0), keepdims=True)
    clip_scale = clip_limit / jnp.maximum(jnp.sqrt(square_sum), clip_limit)

    tile = 32
    tiles = grad.shape[0] // tile
    half = width // 2

    def rows_of(t):
        return pl.ds(pl.multiple_of(t * tile, tile), tile)

    for h in range(2):
        cols = pl.ds(h * half, half)

        def moment(t, tops, cols=cols):
            here = rows_of(t)
            clipped = clip_scale * grad[here, cols]
            first = first_new[here, cols] + (1.0 - beta_first) * clipped
            second = second_new[here, cols] + (1.0 - beta_second) * clipped * clipped
            first_new[here, cols] = first
            second_new[here, cols] = second
            return tuple(
                jnp.maximum(top, jnp.max(value.reshape(tile // 8, 8, half), axis=0))
                for value, top in ((jnp.abs(first), tops[0]), (second, tops[1]))
            )

        tops = lax.fori_loop(0, tiles, moment, (jnp.zeros((8, half), jnp.float32),) * 2)
        for i in range(2):
            colmax[h, i : i + 1, :] = jnp.max(tops[i], axis=0, keepdims=True)
        exchange(colmax.at[h], col_c.at[h], [{C: other}], 2 + h)

    for h in range(2):
        landed(col_c.at[h], small_sem.at[2 + h])
        landed(col_c.at[h], small_send.at[2 + h])
        colmax[h] = jnp.maximum(colmax[h], col_c[h, 0])
        send_spread(colmax.at[h], col_z.at[h], far_first((0,)), 4 + h)

    def direct(t, _):
        here = rows_of(t)
        first, second = first_new[here, :], second_new[here, :]
        direction[here, :] = first / (jnp.sqrt(second) + epsilon)
        for i, value in enumerate((jnp.abs(first), second)):
            most = value[:, :128]
            for j in range(1, width // 128):
                most = jnp.maximum(most, value[:, j * 128 : (j + 1) * 128])
            rowmax[i, here, :] = most
        return _

    lax.fori_loop(0, tiles, direct, 0)
    first_row = jnp.max(jnp.transpose(rowmax[0]), axis=0, keepdims=True)
    first_rowmax[...] = jnp.maximum(first_row, scale_floor)
    second_rowmax[...] = jnp.max(jnp.transpose(rowmax[1]), axis=0, keepdims=True)

    for h in range(2):
        landed(col_z.at[h], small_sem.at[4 + h])
        result = jnp.maximum(colmax[h], jnp.max(col_z[h], axis=0))
        first_colmax[:, h * half : (h + 1) * half] = jnp.maximum(result[0:1], scale_floor)
        second_colmax[:, h * half : (h + 1) * half] = result[1:2]
    landed(norm_p, small_send.at[1])
    for h in range(2):
        spread_done(col_z.at[h], 4 + h)

    landed(got, got_send)
    for kind, (ref, ref_t) in enumerate((
        (sent_l, sent_lt), (sent_m, sent_mt), (sent_l2, sent_l2t), (sent_m2, sent_m2t),
    )):
        landed(ref, sends.at[kind])
        landed(ref_t, sends.at[kind + 4])


def scale(
    direction, first_new, second_new, first_rowmax, first_colmax, second_rowmax, second_colmax,
    direction_out, first_scaled, second_scaled,
    first_row_out, first_col_out, second_row_out, second_col_out,
    out, out_sem, max_sem,
):
    copies = [
        pltpu.make_async_copy(ref, to, max_sem.at[i]) for i, (ref, to) in enumerate((
            (direction, direction_out),
            (first_rowmax, first_row_out), (first_colmax, first_col_out),
            (second_rowmax, second_row_out), (second_colmax, second_col_out),
        ))
    ]
    for copy in copies:
        copy.start()
    rows, width = first_new.shape
    tile = rows // TILES
    for i, (value, row, col, to) in enumerate((
        (first_new, first_rowmax, first_colmax, first_scaled),
        (second_new, second_rowmax, second_colmax, second_scaled),
    )):
        by_row = jnp.transpose(jnp.broadcast_to(1.0 / row[...], (128, rows)))
        by_col = 1.0 / col[...]
        for t in range(TILES):
            here = slice(t * tile, (t + 1) * tile)
            for j in range(width // 128):
                cols = slice(j * 128, j * 128 + 128)
                out[i, here, cols] = value[here, cols] * jnp.maximum(by_row[here], by_col[:, cols])
            copy = pltpu.make_async_copy(out.at[i, here], to.at[here], out_sem.at[t, i])
            copy.start()
            copies.append(copy)
    for copy in copies:
        copy.wait()


def local(
    grad_parts, first_codes, first_rows, first_columns, second_codes, second_rows, second_columns
):
    layer_count, _, row_count, col_count = grad_parts.shape
    entries = layer_count * lax.axis_size(X) * row_count * col_count
    clip_limit = clip_rms * math.sqrt(entries)
    own_rows = first_codes.shape[1]
    rows = own_rows * ACROSS // SLICES
    span = col_count // ACROSS
    q = span // 4
    f32, bf16 = jnp.float32, jnp.bfloat16
    shape = jax.ShapeDtypeStruct
    vmem = pltpu.VMEM
    dma = pltpu.SemaphoreType.DMA
    grads = grad_parts.reshape(2, 2, 2, 2, 2, own_rows, col_count)
    hbm_spec = pl.BlockSpec(memory_space=pltpu.HBM)
    vmem_spec = pl.BlockSpec(memory_space=pltpu.VMEM)
    n = SLICES

    def coded(count):
        return vmem((n, 2, 2, count, rows, q), jnp.int16), vmem((n, 2, 2, count, q), bf16 if count > 1 else f32)

    results = pl.pallas_call(
        functools.partial(kernel, clip_limit),
        out_shape=(
            *[shape((own_rows, col_count), f32)] * 3,
            shape((1, own_rows), f32), shape((1, col_count), f32),
            shape((1, own_rows), f32), shape((1, col_count), f32),
        ),
        in_specs=[hbm_spec] * 7,
        out_specs=[vmem_spec] * 7,
        scratch_shapes=[
            vmem((n, 2, 2, 2, 2, rows, span), bf16),
            vmem((n, 2, 2, 2, 2, rows, span), bf16),
            *coded(8), *coded(8),
            *coded(4), *coded(4),
            vmem((n, 2, 2, 4, rows, q), f32),
            *coded(2), *coded(2),
            *coded(1), *coded(1),
            vmem((2, own_rows, col_count), jnp.int32),
            vmem((own_rows, col_count), f32),
            vmem((8, 128), f32),
            vmem((1, 128), f32),
            vmem((1, 1, 128), f32),
            vmem((127, 1, 128), f32),
            vmem((2, own_rows, 128), f32),
            vmem((2, 2, col_count // 2), f32),
            vmem((2, 1, 2, col_count // 2), f32),
            vmem((2, 15, 2, col_count // 2), f32),
            *[vmem((1, own_rows), f32), vmem((1, col_count), f32)] * 2,
            vmem((1, 16 * (rows + 1) * q), f32),
            vmem((2, 2, 2, 2, rows, span), bf16),
            dma((3,)), dma((n + 4,)), dma((2,)),
            dma((n,)), dma((n,)), dma((n,)), dma((n,)), dma((6,)),
            dma, dma((8,)), dma((6,)), pltpu.SemaphoreType.REGULAR((ROUNDS,)),
        ],
        compiler_params=pltpu.CompilerParams(
            collective_id=0, has_side_effects=True, vmem_limit_bytes=46 * 2**20
        ),
        name="clipped_adam",
    )(
        *(
            pltpu.with_memory_space_constraint(v, pltpu.HBM)
            for v in (
                grads, first_codes[0], first_rows, first_columns, second_codes[0], second_rows,
                second_columns,
            )
        )
    )
    big, by_row, by_col = (shape(s, f32) for s in ((own_rows, col_count), (1, own_rows), (1, col_count)))
    direction, first_scaled, second_scaled, *maxima = pl.pallas_call(
        scale,
        out_shape=(big, big, big, by_row, by_col, by_row, by_col),
        in_specs=[vmem_spec] * 7,
        out_specs=[hbm_spec] * 7,
        scratch_shapes=[vmem((2, own_rows, col_count), f32), dma((TILES, 2)), dma((5,))],
        compiler_params=pltpu.CompilerParams(vmem_limit_bytes=12 * 2**20),
        name="scale",
    )(*results)
    return direction[None], first_scaled[None], second_scaled[None], *maxima


def solution(mesh):
    torus = Mesh(mesh.devices.reshape(mesh.shape["section"], 4, 4, 2), (X, Y, Z, C))
    placed = (
        P(X, FSDP, None, None),
        P(X, FSDP, None),
        P(X, FSDP),
        P(X, None),
        P(X, FSDP, None),
        P(X, FSDP),
        P(X, None),
    )
    return jax.shard_map(
        local,
        mesh=torus,
        in_specs=placed,
        out_specs=(
            P(X, FSDP, None), P(X, FSDP, None), P(X, FSDP, None),
            P(X, FSDP), P(X, None), P(X, FSDP), P(X, None),
        ),
        check_vma=False,
    )
```
